32 devices in a mesh: dp: 16 (over z, x, core), section: 2 (over y).
Axes of the slice: x: 2, y: 2, z: 4, core: 2. Of those that a mesh axis runs over, the one named last changes fastest.
Arguments:
- samples: bfloat16 [128, 512], P('dp'), may hold values from -6 to 6
- targets: bfloat16 [128, 512], P('dp'), may hold values from -6 to 6
- jacobian_targets: bfloat16 [128, 128, 512], P('dp'), may hold values from -0.1796875 to 0.1796875
- directions: int32 [128, 128], P('dp'), may hold values from 0 to 511
- plan: int32 [16, 8], P('dp'), may hold values from 0 to 7, each once within a row
- weights: bfloat16 [2, 512, 8192], P('section'), may hold values from -1 to 1
Outputs:
- gradients: float32 [2, 512, 8192], P('section', 'dp')
The draws below stay inside these ranges and needn't reach their ends.
Inputs may be any that keep to these rules, and one draw needn't show every extreme that they name: `plan`: each row is a permutation of 0 to 7.
All inputs are finite; a program needn't handle non-finite values.
Results may differ from the reference program's by a relative error of at most 0.0034.
Values may be sent and summed in bfloat16 or wider, within the bound.
A program may use at most 128 MiB of HBM per device.

```python
import jax
import jax.numpy as jnp
from jax import lax

REDUCED = 512
WIDTH = 8192
TANGENTS = 128
MICRO = 4
BATCH = 1
POOL = 8
SAMPLES = 128
N_DP = 16


def draw_weights(key, part):
    scales = jnp.array([REDUCED ** (-0.5), WIDTH ** (-0.5)], jnp.float32)[:, None, None]
    base = jnp.clip(jax.random.normal(key, (2, REDUCED, WIDTH), jnp.float32), -4.0, 4.0)
    return (base * scales).astype(jnp.bfloat16)


def place_ends(values, own_key, smallest, largest):
    extent = values.shape
    index_at = [jax.random.randint(jax.random.fold_in(own_key, axis), (), 0, extent[axis]) for axis in range(len(extent))]
    values = values.at[tuple(index_at)].set(smallest)
    longest = extent.index(max(extent))
    index_at[longest] = (index_at[longest] + 1) % extent[longest]
    return values.at[tuple(index_at)].set(largest)


def raised(values, stream_key, source, target, parts, factor):
    owner, partner = [(jnp.arange(values.shape[dim]) // (values.shape[dim] // parts)).reshape([-1 if axis == dim else 1 for axis in range(values.ndim)]) for dim in (source, target)]
    chosen = jax.random.permutation(stream_key, parts)[partner]
    strong = (owner == chosen) | (owner == (partner + parts // 2) % parts)
    return jnp.where(strong, factor * values, values)


def levels(own_key, extent, split, low, largest):
    loudness = 1.0
    for axis_at, parts in split:
        heights = jax.random.uniform(jax.random.fold_in(jax.random.fold_in(own_key, 6), axis_at), (parts,), jnp.float32, low / len(split), largest / len(split))
        loudness = loudness * jnp.repeat(jnp.exp(heights), extent[axis_at] // parts).reshape((-1,) + (1,) * (len(extent) - 1 - axis_at))
    return loudness


def gaussian(stream_key, extent, spread, most, split=(), held_as=jnp.bfloat16):
    loudness = levels(stream_key, extent, split, -0.22, 0.18) if split else 1.0
    result = jax.random.normal(stream_key, extent, jnp.float32) * spread * loudness
    return jnp.minimum(jnp.maximum(result, -most), most).astype(held_as)


def gaussian_with(stream_key, extent, scale, bound, pieces, heavy, kind=jnp.bfloat16):
    entries = scale * jax.random.normal(stream_key, extent, jnp.float32)
    if pieces:
        entries = entries * levels(stream_key, extent, pieces, -0.22, 0.18)
    return jnp.clip(raised(entries, jax.random.fold_in(stream_key, 3), *heavy), -bound, bound).astype(kind)


def setup_inputs(seed: int = 0) -> dict:
    arg_keys = jax.random.split(jax.random.key(seed), 7)
    samples = gaussian_with(arg_keys[0], (SAMPLES, REDUCED), 1.0, 6.0, ((0, 16),), (0, 1, 16, 2.0))
    targets = gaussian_with(arg_keys[1], (SAMPLES, REDUCED), 1.0, 6.0, ((0, 16),), (0, 1, 16, 2.0))
    jacobian_targets = gaussian(arg_keys[2], (SAMPLES, TANGENTS, REDUCED), 0.03, 0.1796875, ((0, 16),))
    directions = place_ends(jax.random.randint(arg_keys[3], (SAMPLES, TANGENTS), 0, REDUCED), jax.random.fold_in(arg_keys[3], 1), 0, REDUCED - 1).astype(jnp.int32)
    plan = jax.vmap(lambda own: jax.random.permutation(own, POOL))(jax.random.split(arg_keys[4], N_DP)).reshape((N_DP, POOL)).astype(jnp.int32)
    weights = draw_weights(jax.random.fold_in(arg_keys[6], 71), 0)
    return dict(samples=samples, targets=targets, jacobian_targets=jacobian_targets, directions=directions, plan=plan, weights=weights)


jacobian_weight = 32.0


def contract_rows(left, right):
    return lax.dot_general(left, right, (((0,), (0,)), ((), ())), preferred_element_type=jnp.float32)


def against_rows(left, right):
    return lax.dot_general(left, right, (((1,), (1,)), ((), ())), preferred_element_type=jnp.float32)


def encoder_parts(inputs, chosen_dirs, w_first):
    linear = jnp.dot(inputs, w_first, preferred_element_type=jnp.float32)
    squash = jax.nn.sigmoid(linear)
    first_slope = squash * (1.0 + linear * (1.0 - squash))
    second_slope = squash * (1.0 - squash) * (2.0 + linear * (1.0 - 2.0 * squash))
    picked = jnp.take(w_first, chosen_dirs, axis=0)
    return linear, squash, first_slope, second_slope, picked


def encoder_forward(encoded):
    linear, squash, first_slope, second_slope, picked = encoded
    hidden = (linear * squash).astype(jnp.bfloat16)
    tangent = (first_slope[:, None, :] * picked.astype(jnp.float32)).astype(jnp.bfloat16)
    return hidden, tangent


def decoder(hidden, tangent, w_last, target_rows, jacobian_rows):
    columns = hidden.shape[1]
    flattened = tangent.reshape(-1, columns)
    output = against_rows(hidden, w_last)
    jacobian = against_rows(flattened, w_last)
    misfit = (output - target_rows.astype(jnp.float32)).astype(jnp.bfloat16)
    jac_misfit = (jacobian_weight * (jacobian - jacobian_rows.reshape(jacobian.shape).astype(jnp.float32))).astype(jnp.bfloat16)
    grad_last = contract_rows(misfit, hidden) + contract_rows(jac_misfit, flattened)
    cotangent = jnp.dot(misfit, w_last, preferred_element_type=jnp.float32).astype(jnp.bfloat16)
    cotangent_tangent = jnp.dot(jac_misfit, w_last, preferred_element_type=jnp.float32).astype(jnp.bfloat16)
    return grad_last, cotangent, cotangent_tangent.reshape(tangent.shape)


def encoder_backward(inputs, chosen_dirs, encoded, cotangent, cotangent_tangent, reduced):
    linear, squash, first_slope, second_slope, picked = encoded
    projected = jnp.sum(cotangent_tangent.astype(jnp.float32) * picked.astype(jnp.float32), axis=1)
    grad_pre = (cotangent.astype(jnp.float32) * first_slope + second_slope * projected).astype(jnp.bfloat16)
    grad_picked = (cotangent_tangent.astype(jnp.float32) * first_slope[:, None, :]).astype(jnp.bfloat16)
    columns = grad_pre.shape[1]
    onehot = (chosen_dirs.reshape(-1)[:, None] == jnp.arange(reduced, dtype=jnp.int32)[None, :]).astype(jnp.bfloat16)
    return contract_rows(inputs, grad_pre) + contract_rows(onehot, grad_picked.reshape(-1, columns))


def reference(samples, targets, jacobian_targets, directions, plan, weights):
    w_first = weights[0]
    w_last = weights[1]
    offsets = jnp.arange(N_DP, dtype=jnp.int32) * POOL
    picked_rows = (plan[:, :MICRO * BATCH].astype(jnp.int32) + offsets[:, None]).reshape(-1).astype(jnp.int32)

    def accumulate(carried, position):
        first_total, last_total = carried
        inputs = lax.dynamic_slice_in_dim(samples, position, 1, 0)
        chosen_dirs = lax.dynamic_slice_in_dim(directions, position, 1, 0)
        target_rows = lax.dynamic_slice_in_dim(targets, position, 1, 0)
        jacobian_rows = lax.dynamic_slice_in_dim(jacobian_targets, position, 1, 0)
        encoded = encoder_parts(inputs, chosen_dirs, w_first)
        hidden, tangent = encoder_forward(encoded)
        grad_last, cotangent, cotangent_tangent = decoder(hidden, tangent, w_last, target_rows, jacobian_rows)
        grad_first = encoder_backward(inputs, chosen_dirs, encoded, cotangent, cotangent_tangent, REDUCED)
        return (first_total + grad_first, last_total + grad_last), None

    cleared = jnp.zeros((REDUCED, WIDTH), jnp.float32)
    totals, unused = lax.scan(accumulate, (cleared, cleared), picked_rows)
    return jnp.stack([totals[0], totals[1]])
```

```python
import functools

import jax
import jax.numpy as jnp
from jax import lax
from jax.experimental import pallas as pl
from jax.experimental.pallas import tpu as pltpu
from jax.sharding import PartitionSpec as P

MICRO = 4
GROUP = 4
PAD = 16
PIECES = 8
CHUNKS = 4
STRIPS = 4
QUADS = 4

jacobian_weight = 32.0

VMEM = pl.BlockSpec(memory_space=pltpu.VMEM)
ANY = pl.BlockSpec(memory_space=pl.ANY)


def remote(src, dst, send, recv, dp, sec):
    return pltpu.make_async_remote_copy(
        src_ref=src, dst_ref=dst, send_sem=send, recv_sem=recv,
        device_id={"dp": dp, "section": sec},
    )


def fused_kernel(
    n_s, plan, samples, directions, targets, jac_hbm, weight, out,
    packs, both, jac, xs, dirs, onehot_t, onehot, act, hidden, picked, first, second,
    partial, first_in, sums, second_in, misfit, total, grads, inbox, halves,
    last_total, last_grads, last_inbox, last_halves, pulled, proj, finished,
    psend, precv, wsend, wrecv, zsend, zrecv, s1, r1, s2, r2, s3, r3, s4, r4,
    s5, r5, s6, r6, s7, r7, local,
):
    f32, bf16 = jnp.float32, jnp.bfloat16
    dp, sec = lax.axis_index("dp"), lax.axis_index("section")
    g = lax.rem(dp, GROUP)
    base = dp - g
    s = dp // GROUP
    core, half = lax.rem(g, 2), g // 2
    q = sec * 2 + half
    mine = core * QUADS + q
    partner = (base + half * 2 + (1 - core), sec)
    parity = lax.rem(s, 2)
    mate = s + 1 - 2 * parity
    twin = (mate * GROUP + g, sec)
    line = n_s == 4
    reduced, cols = both.shape[1:]
    tangents = directions.shape[1]
    spt = MICRO // 2
    rows = spt * tangents
    strip = reduced // STRIPS
    slab = reduced // n_s
    own_rows = slab // GROUP
    cw = cols // CHUNKS
    pw = cols // PIECES
    over_rows = (((0,), (0,)), ((), ()))
    over_cols = (((1,), (1,)), ((), ()))

    def quad(k):
        l = 1 - sec if k & 2 else sec
        h = 1 - half if k & 1 else half
        return l * 2 + h, (base + h * 2 + core, l)

    if line:
        opposite = lax.rem(s + 2, 4)
        mate_opposite = lax.rem(mate + 2, 4)
        others = [mate, opposite]
        order = [mate_opposite, opposite, mate, s]
        pairs = [1 - s // 2, s // 2]
    else:
        others = [lax.rem(s + k, n_s) for k in range(1, n_s)]
        order = list(range(STRIPS))
        pairs = [0, 1]

    own = pltpu.make_async_copy(
        weight.at[0, :, pl.ds(pl.multiple_of((sec * GROUP + g) * cols, cols), cols)],
        both.at[sec], local.at[0],
    )
    own.start()
    load_jac = pltpu.make_async_copy(jac_hbm, jac, local.at[1])
    load_jac.start()

    barrier = pltpu.get_barrier_semaphore()
    peers = [
        (base + lax.rem(g + k, GROUP), 1 - sec if j else sec)
        for j in range(2) for k in range(GROUP) if j or k
    ] + [(o * GROUP + g, sec) for o in others]
    for d, l in peers:
        pl.semaphore_signal(barrier, inc=1, device_id={"dp": d, "section": l})
    pl.semaphore_wait(barrier, len(peers))

    half_rows = pl.ds(pl.multiple_of(parity * (reduced // 2), reduced // 2), reduced // 2)
    far_start = pl.multiple_of(((1 - sec) * GROUP + g) * cols, cols)
    sent, relayed = [], []
    for c in range(PIECES):
        sent.append(remote(
            weight.at[0, half_rows, pl.ds(far_start + c * pw, pw)],
            both.at[sec, half_rows, pl.ds(c * pw, pw)],
            wsend.at[c], wrecv.at[c], dp, 1 - sec,
        ))
        sent[-1].start()

    every = jnp.concatenate(
        [samples[...].astype(f32), directions[...].astype(f32)], axis=1
    )
    row = lax.broadcasted_iota(jnp.int32, every.shape, 0)
    packed = jnp.zeros_like(every)
    for k in range(MICRO):
        chosen = jnp.sum(jnp.where(row == plan[0, k], every, 0.0), axis=0, keepdims=True)
        packed = jnp.where(row == k, chosen, packed)
    packs[g] = packed
    shared = []
    for k in range(1, GROUP):
        shared.append(remote(
            packs.at[g], packs.at[g], psend.at[k - 1], precv.at[k - 1],
            base + lax.rem(g + k, GROUP), sec,
        ))
        shared[-1].start()
    for copy in shared:
        copy.wait_recv()
    for b in range(2 * QUADS):
        c, l, h = b // QUADS, (b % QUADS) // 2, b % 2
        xs[b * spt : (b + 1) * spt] = packs[h * 2 + c, l * spt : (l + 1) * spt, :reduced]
        dirs[b * spt : (b + 1) * spt] = packs[h * 2 + c, l * spt : (l + 1) * spt, reduced:]
    n_all = 2 * QUADS * spt
    turned = dirs[...].T
    for t in range(n_all):
        lane = lax.broadcasted_iota(jnp.int32, (tangents, reduced), 1).astype(f32)
        onehot_t[t * tangents : (t + 1) * tangents] = (
            (lane == turned[:, t : t + 1]).astype(f32).astype(bf16)
        )

    n_loop = 2
    loop_rows = n_all * tangents // n_loop
    loop_samples = n_all // n_loop

    def forward(c):
        lo, hi = c * cw, (c + 1) * cw
        linear = jnp.dot(xs[...].astype(bf16), both[0, :, lo:hi], preferred_element_type=f32)
        squash = jax.nn.sigmoid(linear)
        first[:, lo:hi] = squash * (1.0 + linear * (1.0 - squash))
        second[:, lo:hi] = squash * (1.0 - squash) * (2.0 + linear * (1.0 - 2.0 * squash))
        hidden[:, lo:hi] = (linear * squash).astype(bf16)

        def pick(i, carry):
            start = pl.multiple_of(i * loop_rows, loop_rows)
            value = jnp.dot(
                onehot_t[pl.ds(start, loop_rows), :], both[0, :, lo:hi],
                preferred_element_type=f32,
            )
            picked[pl.ds(start, loop_rows), lo:hi] = value.astype(bf16)
            for t in range(loop_samples):
                slope = first[pl.ds(i * loop_samples + t, 1), lo:hi]
                here = pl.ds(pl.multiple_of(start + t * tangents, tangents), tangents)
                act[here, lo:hi] = (
                    slope * value[t * tangents : (t + 1) * tangents]
                ).astype(bf16)
            return carry

        lax.fori_loop(0, n_loop, pick, 0)

    own.wait()
    per_chunk = PIECES // CHUNKS

    def arrive(c):
        for i in range(c * per_chunk, (c + 1) * per_chunk):
            sent[i].wait_recv()
            came = both.at[1 - sec, half_rows, pl.ds(i * pw, pw)]
            relayed.append(remote(came, came, zsend.at[i], zrecv.at[i], *twin))
            relayed[-1].start()

    def complete(c):
        for i in range(c * per_chunk, (c + 1) * per_chunk):
            relayed[i].wait_recv()

    for c in range(CHUNKS):
        arrive(c)
        if c:
            complete(c - 1)
            forward(c - 1)
    complete(CHUNKS - 1)
    forward(CHUNKS - 1)

    def partials(pair, side):
        start = pl.multiple_of(pair * 2 * strip, 2 * strip)
        decoder = both[1, pl.ds(start, 2 * strip), :]
        lo = pl.multiple_of(side * (QUADS * rows), QUADS * rows)
        value = lax.dot_general(
            act[pl.ds(lo, QUADS * rows), :], decoder, over_cols, preferred_element_type=f32
        ).astype(bf16)
        tail = lax.dot_general(
            hidden[...], decoder, over_cols, preferred_element_type=f32
        ).astype(bf16)
        for i in range(2):
            a, b = i * strip, (i + 1) * strip
            for j in range(QUADS):
                partial[pair * 2 + i, side * QUADS + j, 0:rows] = (
                    value[j * rows : (j + 1) * rows, a:b]
                )
                partial[pair * 2 + i, side * QUADS + j, rows:] = tail[:, a:b]

    def across(p):
        theirs = pl.ds(pl.multiple_of((1 - core) * QUADS, QUADS), QUADS)
        return remote(
            partial.at[p, theirs], first_in.at[p], s1.at[p], r1.at[p], *partner
        )

    def away(p, k):
        return remote(
            sums.at[p, k - 1], second_in.at[p, k - 1],
            s2.at[p * 3 + k - 1], r2.at[p * 3 + k - 1], *quad(k)[1],
        )

    def gather(p, k):
        if k == 0:
            return remote(
                misfit.at[p, mine], misfit.at[p, mine], s4.at[p * 4], r4.at[p * 4], *partner
            )
        return remote(
            misfit.at[p, mine], misfit.at[p, mine],
            s3.at[p * 3 + k - 1], r3.at[p * 3 + k - 1], *quad(k)[1],
        )

    def passing(p, k):
        came = misfit.at[p, core * QUADS + quad(k)[0]]
        return remote(came, came, s4.at[p * 4 + k], r4.at[p * 4 + k], *partner)

    def reduce_out(p):
        across(p).wait_recv()
        for k in (3, 1, 2):
            other = quad(k)[0]
            sums[p, k - 1] = (
                partial[p, core * QUADS + other].astype(f32) + first_in[p, other].astype(f32)
            ).astype(bf16)
            away(p, k).start()

    def compare(p):
        for k in range(1, QUADS):
            away(p, k).wait_recv()
        lanes = pl.ds(pl.multiple_of(p * strip, strip), strip)

        def whole(lo, hi):
            value = partial[p, mine, lo:hi].astype(f32) + first_in[p, q, lo:hi].astype(f32)
            for k in range(1, QUADS):
                value = value + second_in[p, k - 1, lo:hi].astype(f32)
            return value

        all_targets = targets[:, lanes].astype(f32)
        pool_row = lax.broadcasted_iota(jnp.int32, all_targets.shape, 0)
        tail_row = lax.broadcasted_iota(jnp.int32, (PAD, strip), 0)
        tail = jnp.zeros((PAD, strip), f32)
        outputs = whole(rows, rows + PAD)
        for i in range(spt):
            lo, hi = i * tangents, (i + 1) * tangents
            index = plan[0, sec * spt + i]
            misfit[p, mine, lo:hi] = (
                jacobian_weight * (whole(lo, hi) - jac[index, :, lanes].astype(f32))
            ).astype(bf16)
            target = jnp.sum(
                jnp.where(pool_row == index, all_targets, 0.0), axis=0, keepdims=True
            )
            tail = jnp.where(tail_row == mine * spt + i, outputs - target, tail)
        misfit[p, mine, rows:] = tail.astype(bf16)
        for k in (3, 1, 2, 0):
            gather(p, k).start()

    def pass_on(p):
        for k in (1, 2, 3):
            gather(p, k).wait_recv()
            passing(p, k).start()

    def last_of(p):
        for k in range(QUADS):
            (passing(p, k) if k else gather(p, 0)).wait_recv()
        lhs = jnp.concatenate([misfit[p, b, 0:rows] for b in range(2 * QUADS)], axis=0)
        value = lax.dot_general(lhs, act[...], over_rows, preferred_element_type=f32)
        tail = misfit[p, 0, rows:].astype(f32)
        for b in range(1, 2 * QUADS):
            tail = tail + misfit[p, b, rows:].astype(f32)
        value = value + lax.dot_general(
            tail.astype(bf16), hidden[...], over_rows, preferred_element_type=f32
        )
        here = pl.ds(pl.multiple_of(p * strip, strip), strip)
        last_total[here, :] = value
        last_grads[here, :] = value.astype(bf16)

    def slab_of(o):
        return pl.ds(pl.multiple_of(o * slab, slab), slab)

    def last_link(kind):
        if not line:
            o = others[kind]
            source = last_grads.at[slab_of(o), :]
        elif kind == 2:
            o, source = opposite, last_halves
        else:
            o, source = mate, last_grads.at[slab_of([mate_opposite, mate][kind]), :]
        return remote(
            source, last_inbox.at[kind], s5.at[kind], r5.at[kind], o * GROUP + g, sec
        )

    def last_relay():
        last_link(0).wait_recv()
        last_halves[...] = (
            last_total[slab_of(opposite), :] + last_inbox[0].astype(f32)
        ).astype(bf16)
        last_link(2).start()

    def link(j, kind):
        if not line:
            o = others[kind]
            source = grads.at[j, slab_of(o), :]
        elif kind == 2:
            o, source = opposite, halves.at[j]
        else:
            o, source = mate, grads.at[j, slab_of([mate_opposite, mate][kind]), :]
        i = j * inbox.shape[1] + kind
        return remote(source, inbox.at[j, kind], s6.at[i], r6.at[i], o * GROUP + g, sec)

    def relay(j):
        link(j, 0).wait_recv()
        halves[j] = (
            total[j, slab_of(opposite), :] + inbox[j, 0].astype(f32)
        ).astype(bf16)
        link(j, 2).start()

    def columns(j):
        start = pl.multiple_of((sec * GROUP + g) * cols + j * cw, cw)
        return out.at[:, pl.ds(start, cw)]

    def hand(layer, j, k):
        h = lax.rem(g + k, GROUP)
        i = j * 2 * GROUP
        return remote(
            finished.at[layer, j, h], columns(j),
            s7.at[layer * CHUNKS * GROUP + j * GROUP + k], r7.at[i + sec * GROUP + k],
            base + h, layer,
        )

    kinds = range(1, 3) if line else range(n_s - 1)

    def finish(layer, j):
        for h in range(GROUP):
            start = pl.multiple_of(s * slab + h * own_rows, own_rows)
            here = slice(h * own_rows, (h + 1) * own_rows)
            if layer:
                lo, hi = j * cw, (j + 1) * cw
                value = last_total[pl.ds(start, own_rows), lo:hi]
                for k in kinds:
                    value = value + last_inbox[k, here, lo:hi].astype(f32)
            else:
                value = total[j, pl.ds(start, own_rows), :]
                for k in kinds:
                    value = value + inbox[j, k, here, :].astype(f32)
            finished[layer, j, h] = value.astype(bf16)
        for k in range(1, GROUP):
            hand(layer, j, k).start()

        @pl.when(sec != layer)
        def _():
            hand(layer, j, 0).start()

        @pl.when(sec == layer)
        def _():
            columns(j)[...] = finished[layer, j, g]

    def backward(j):
        lo, hi = j * cw, (j + 1) * cw

        def pull(i, carry):
            lhs = jnp.concatenate(
                [
                    jnp.concatenate(
                        [misfit[p, i * QUADS + b, 0:rows] for p in range(STRIPS)], axis=1
                    )
                    for b in range(QUADS)
                ],
                axis=0,
            )
            cot = jnp.dot(lhs, both[1, :, lo:hi], preferred_element_type=f32)
            start = pl.multiple_of(i * loop_rows, loop_rows)
            for t in range(loop_samples):
                part = cot[t * tangents : (t + 1) * tangents]
                here = pl.ds(pl.multiple_of(start + t * tangents, tangents), tangents)
                slope = first[pl.ds(i * loop_samples + t, 1), lo:hi]
                proj[pl.ds(i * loop_samples + t, 1), :] = jnp.sum(
                    part * picked[here, lo:hi].astype(f32), axis=0, keepdims=True
                )
                pulled[here, :] = (part * slope).astype(bf16)
            return carry

        lax.fori_loop(0, n_loop, pull, 0)
        tail = jnp.zeros((PAD, reduced), f32)
        for b in range(2 * QUADS):
            tail = tail + jnp.concatenate(
                [misfit[p, b, rows:] for p in range(STRIPS)], axis=1
            ).astype(f32)
        cot = jnp.dot(tail.astype(bf16), both[1, :, lo:hi], preferred_element_type=f32)
        pre = (cot * first[:, lo:hi] + second[:, lo:hi] * proj[...]).astype(bf16)
        value = jnp.dot(onehot[...], pulled[...], preferred_element_type=f32)
        value = value + lax.dot_general(
            xs[...].astype(bf16), pre, over_rows, preferred_element_type=f32
        )
        total[j] = value
        grads[j] = value.astype(bf16)

    for i in range(2):
        partials(pairs[i], 1 - core)
        across(order[2 * i]).start()
        across(order[2 * i + 1]).start()
        partials(pairs[i], core)
    reduce_out(order[0])
    reduce_out(order[1])
    for t in range(n_all):
        deep = lax.broadcasted_iota(jnp.int32, (reduced, tangents), 0).astype(f32)
        onehot[:, t * tangents : (t + 1) * tangents] = (
            (deep == dirs[t : t + 1, :]).astype(f32).astype(bf16)
        )
    load_jac.wait()
    compare(order[0])
    reduce_out(order[2])
    compare(order[1])
    reduce_out(order[3])
    pass_on(order[0])
    compare(order[2])
    last_of(order[0])
    if line:
        last_link(0).start()
    pass_on(order[1])
    compare(order[3])
    last_of(order[1])
    pass_on(order[2])
    if line:
        last_relay()
    last_of(order[2])
    if line:
        last_link(1).start()
    pass_on(order[3])
    if line:
        for k in range(QUADS):
            (passing(order[3], k) if k else gather(order[3], 0)).wait_recv()
    else:
        last_of(order[3])
        for kind in range(n_s - 1):
            last_link(kind).start()
    for j in range(CHUNKS):
        backward(j)
        if line:
            link(j, 0).start()
            link(j, 1).start()
            if j >= 2:
                relay(j - 2)
        else:
            for kind in range(n_s - 1):
                link(j, kind).start()
    if line:
        relay(CHUNKS - 2)
        lhs = jnp.concatenate(
            [misfit[order[3], b, 0:rows] for b in range(2 * QUADS)], axis=0
        )
        value = lax.dot_general(lhs, act[...], over_rows, preferred_element_type=f32)
        tail = misfit[order[3], 0, rows:].astype(f32)
        for b in range(1, 2 * QUADS):
            tail = tail + misfit[order[3], b, rows:].astype(f32)
        last_total[slab_of(s), :] = value + lax.dot_general(
            tail.astype(bf16), hidden[...], over_rows, preferred_element_type=f32
        )
        relay(CHUNKS - 1)
    for k in kinds:
        last_link(k).wait_recv()
    for j in range(CHUNKS):
        finish(1, j)
    for j in range(CHUNKS):
        for k in kinds:
            link(j, k).wait_recv()
        finish(0, j)

    for copy in shared + sent + relayed:
        copy.wait_send()
    for p in range(STRIPS):
        across(p).wait_send()
        for k in range(1, QUADS):
            away(p, k).wait_send()
            passing(p, k).wait_send()
        for k in range(QUADS):
            gather(p, k).wait_send()
    for k in range(last_inbox.shape[0]):
        last_link(k).wait_send()
        for j in range(CHUNKS):
            link(j, k).wait_send()
    for layer in range(2):
        for j in range(CHUNKS):
            for k in range(1, GROUP):
                hand(layer, j, k).wait_send()

            @pl.when(sec != layer)
            def _():
                hand(layer, j, 0).wait_send()

    for j in range(CHUNKS):
        for i in range(2):
            for k in range(GROUP):
                at = j * 2 * GROUP + i * GROUP + k
                arrival = remote(
                    finished.at[0, j, 0], columns(j), s7.at[0], r7.at[at], *partner
                )
                if k:
                    arrival.wait_recv()
                else:

                    @pl.when(sec != i)
                    def _():
                        arrival.wait_recv()


def shards(n_dp, n_sec, samples, targets, jacobian_targets, directions, plan, weights):
    _, reduced, width = weights.shape
    pool, tangents = directions.shape
    team = n_sec * GROUP
    cols = width // team
    n_s = n_dp // GROUP
    spt = MICRO // n_sec
    rows = spt * tangents
    high = rows + PAD
    every = team * spt
    strip = reduced // STRIPS
    slab = reduced // n_s
    cw = cols // CHUNKS
    kinds = 3 if n_s == 4 else n_s - 1
    f32, bf16 = jnp.float32, jnp.bfloat16
    vmem = pltpu.VMEM
    dma = lambda n: pltpu.SemaphoreType.DMA((n,))
    result = pl.pallas_call(
        functools.partial(fused_kernel, n_s),
        out_shape=jax.ShapeDtypeStruct((reduced // n_dp, width), bf16),
        in_specs=[pl.BlockSpec(memory_space=pltpu.SMEM), VMEM, VMEM, VMEM, ANY, ANY],
        out_specs=VMEM,
        scratch_shapes=[
            vmem((GROUP, pool, reduced + tangents), f32),
            vmem((n_sec, reduced, cols), bf16),
            vmem(jacobian_targets.shape, bf16),
            vmem((every, reduced), f32),
            vmem((every, tangents), f32),
            vmem((every * tangents, reduced), bf16),
            vmem((reduced, every * tangents), bf16),
            vmem((every * tangents, cols), bf16),
            vmem((every, cols), bf16),
            vmem((every * tangents, cols), bf16),
            vmem((every, cols), f32),
            vmem((every, cols), f32),
            vmem((STRIPS, team, high, strip), bf16),
            vmem((STRIPS, QUADS, high, strip), bf16),
            vmem((STRIPS, QUADS - 1, high, strip), bf16),
            vmem((STRIPS, QUADS - 1, high, strip), bf16),
            vmem((STRIPS, team, high, strip), bf16),
            vmem((CHUNKS, reduced, cw), f32),
            vmem((CHUNKS, reduced, cw), bf16),
            vmem((CHUNKS, kinds, slab, cw), bf16),
            vmem((CHUNKS, slab, cw), bf16),
            vmem((reduced, cols), f32),
            vmem((reduced, cols), bf16),
            vmem((kinds, slab, cols), bf16),
            vmem((slab, cols), bf16),
            vmem((every * tangents, cw), bf16),
            vmem((every, cw), f32),
            vmem((n_sec, CHUNKS, GROUP, reduced // n_dp, cw), bf16),
            dma(GROUP - 1), dma(GROUP - 1), dma(PIECES), dma(PIECES), dma(PIECES), dma(PIECES),
            dma(STRIPS), dma(STRIPS), dma(STRIPS * 3), dma(STRIPS * 3),
            dma(STRIPS * 3), dma(STRIPS * 3), dma(STRIPS * 4), dma(STRIPS * 4),
            dma(kinds), dma(kinds), dma(CHUNKS * kinds), dma(CHUNKS * kinds),
            dma(2 * CHUNKS * GROUP), dma(2 * CHUNKS * GROUP), dma(2),
        ],
        compiler_params=pltpu.CompilerParams(
            collective_id=0, has_side_effects=True, vmem_limit_bytes=60 * 1024 * 1024
        ),
        name="fused",
    )(plan, samples, directions, targets, jacobian_targets, weights)
    return result.astype(f32)[None]


def solution(mesh):
    placed = (
        P("dp", None),
        P("dp", None),
        P("dp", None, None),
        P("dp", None),
        P("dp", None),
        P("section", None, None),
    )
    body = functools.partial(shards, mesh.shape["dp"], mesh.shape["section"])
    return jax.shard_map(
        body, mesh=mesh, in_specs=placed, out_specs=P("section", "dp", None), check_vma=False
    )
```

```python
import functools

import jax
import jax.numpy as jnp
from jax import lax
from jax.experimental import pallas as pl
from jax.experimental.pallas import tpu as pltpu
from jax.sharding import PartitionSpec as P

MICRO = 4
GROUP = 4
PAD = 16
PIECES = 8
CHUNKS = 4
STRIPS = 4
LINKS = 8
LASTS = 2
QUADS = 4

jacobian_weight = 32.0

VMEM = pl.BlockSpec(memory_space=pltpu.VMEM)
ANY = pl.BlockSpec(memory_space=pl.ANY)


def remote(src, dst, send, recv, dp, sec):
    return pltpu.make_async_remote_copy(
        src_ref=src, dst_ref=dst, send_sem=send, recv_sem=recv,
        device_id={"dp": dp, "section": sec},
    )


def fused_kernel(
    n_s, plan, samples, directions, targets, jac_hbm, weight, out,
    packs, both, mail, jac, xs, dirs, onehot_t, onehot, act, hidden, picked, first, second,
    partial, first_in, sums, second_in, misfit, total, grads, inbox, halves,
    last_total, last_grads, last_inbox, last_halves, pulled, proj, finished,
    psend, precv, wsend, wrecv, zsend, zrecv, s1, r1, s2, r2, s3, r3, s4, r4,
    s5, r5, s6, r6, s7, r7, local,
):
    f32, bf16 = jnp.float32, jnp.bfloat16
    dp, sec = lax.axis_index("dp"), lax.axis_index("section")
    g = lax.rem(dp, GROUP)
    base = dp - g
    s = dp // GROUP
    core, half = lax.rem(g, 2), g // 2
    q = sec * 2 + half
    mine = core * QUADS + q
    partner = (base + half * 2 + (1 - core), sec)
    parity = lax.rem(s, 2)
    mate = s + 1 - 2 * parity
    twin = (mate * GROUP + g, sec)
    line = n_s == 4
    reduced, cols = both.shape[1:]
    tangents = directions.shape[1]
    spt = MICRO // 2
    rows = spt * tangents
    strip = reduced // STRIPS
    slab = reduced // n_s
    own_rows = slab // GROUP
    cw = cols // CHUNKS
    pw = cols // PIECES
    zw = cols // LINKS
    lw = cols // LASTS
    over_rows = (((0,), (0,)), ((), ()))
    over_cols = (((1,), (1,)), ((), ()))

    def quad(k):
        l = 1 - sec if k & 2 else sec
        h = 1 - half if k & 1 else half
        return l * 2 + h, (base + h * 2 + core, l)

    if line:
        opposite = lax.rem(s + 2, 4)
        mate_opposite = lax.rem(mate + 2, 4)
        others = [mate, opposite]
        order = [mate_opposite, opposite, mate, s]
        pairs = [1 - s // 2, s // 2]
    else:
        others = [lax.rem(s + k, n_s) for k in range(1, n_s)]
        order = list(range(STRIPS))
        pairs = [0, 1]

    far_start = pl.multiple_of(((1 - sec) * GROUP + g) * cols, cols)
    load_mail = pltpu.make_async_copy(
        weight.at[0, :, pl.ds(far_start, cols)], mail, local.at[2]
    )
    load_mail.start()
    own = pltpu.make_async_copy(
        weight.at[0, :, pl.ds(pl.multiple_of((sec * GROUP + g) * cols, cols), cols)],
        both.at[sec], local.at[0],
    )
    own.start()
    load_jac = pltpu.make_async_copy(jac_hbm, jac, local.at[1])
    load_jac.start()

    barrier = pltpu.get_barrier_semaphore()
    peers = [
        (base + lax.rem(g + k, GROUP), 1 - sec if j else sec)
        for j in range(2) for k in range(GROUP) if j or k
    ] + [(o * GROUP + g, sec) for o in others]
    for d, l in peers:
        pl.semaphore_signal(barrier, inc=1, device_id={"dp": d, "section": l})
    pl.semaphore_wait(barrier, len(peers))

    side = reduced // 2
    half_rows = pl.ds(pl.multiple_of(parity * side, side), side)
    other_rows = pl.ds(pl.multiple_of((1 - parity) * side, side), side)
    load_mail.wait()
    sent, relayed = [], []
    for c in range(PIECES + 1):
        here = (half_rows if c < PIECES else other_rows, pl.ds(min(c, PIECES - 1) * pw, pw))
        sent.append(remote(
            mail.at[here], both.at[(sec,) + here], wsend.at[c], wrecv.at[c], dp, 1 - sec,
        ))
        sent[-1].start()

    every = jnp.concatenate(
        [samples[...].astype(f32), directions[...].astype(f32)], axis=1
    )
    row = lax.broadcasted_iota(jnp.int32, every.shape, 0)
    packed = jnp.zeros_like(every)
    for k in range(MICRO):
        chosen = jnp.sum(jnp.where(row == plan[0, k], every, 0.0), axis=0, keepdims=True)
        packed = jnp.where(row == k, chosen, packed)
    packs[g] = packed
    shared = []
    for k in range(1, GROUP):
        shared.append(remote(
            packs.at[g], packs.at[g], psend.at[k - 1], precv.at[k - 1],
            base + lax.rem(g + k, GROUP), sec,
        ))
        shared[-1].start()

    def arrive(c):
        sent[c].wait_recv()
        if c < PIECES - 1:
            came = both.at[1 - sec, half_rows, pl.ds(c * pw, pw)]
            relayed.append(remote(came, came, zsend.at[c], zrecv.at[c], *twin))
            relayed[-1].start()

    arrive(0)
    for copy in shared:
        copy.wait_recv()
    for b in range(2 * QUADS):
        c, l, h = b // QUADS, (b % QUADS) // 2, b % 2
        xs[b * spt : (b + 1) * spt] = packs[h * 2 + c, l * spt : (l + 1) * spt, :reduced]
        dirs[b * spt : (b + 1) * spt] = packs[h * 2 + c, l * spt : (l + 1) * spt, reduced:]
    n_all = 2 * QUADS * spt
    turned = dirs[...].T

    def spread_directions(ts):
        for t in ts:
            lane = lax.broadcasted_iota(jnp.int32, (tangents, reduced), 1).astype(f32)
            onehot_t[t * tangents : (t + 1) * tangents] = (
                (lane == turned[:, t : t + 1]).astype(f32).astype(bf16)
            )

    arrive(1)
    spread_directions(range(n_all // 2))
    arrive(2)
    spread_directions(range(n_all // 2, n_all))
    arrive(3)

    n_loop = 2
    loop_rows = n_all * tangents // n_loop
    loop_samples = n_all // n_loop

    def forward(c):
        lo, hi = c * cw, (c + 1) * cw
        linear = jnp.dot(xs[...].astype(bf16), both[0, :, lo:hi], preferred_element_type=f32)
        squash = jax.nn.sigmoid(linear)
        first[:, lo:hi] = squash * (1.0 + linear * (1.0 - squash))
        second[:, lo:hi] = squash * (1.0 - squash) * (2.0 + linear * (1.0 - 2.0 * squash))
        hidden[:, lo:hi] = (linear * squash).astype(bf16)

        def pick(i, carry):
            start = pl.multiple_of(i * loop_rows, loop_rows)
            value = jnp.dot(
                onehot_t[pl.ds(start, loop_rows), :], both[0, :, lo:hi],
                preferred_element_type=f32,
            )
            picked[pl.ds(start, loop_rows), lo:hi] = value.astype(bf16)
            for t in range(loop_samples):
                slope = first[pl.ds(i * loop_samples + t, 1), lo:hi]
                here = pl.ds(pl.multiple_of(start + t * tangents, tangents), tangents)
                act[here, lo:hi] = (
                    slope * value[t * tangents : (t + 1) * tangents]
                ).astype(bf16)
            return carry

        lax.fori_loop(0, n_loop, pick, 0)

    own.wait()
    per_chunk = PIECES // CHUNKS
    for c in range(CHUNKS):
        for i in ([], [4, 5], [6], [7, 8])[c]:
            arrive(i)
        for i in range(c * per_chunk, min((c + 1) * per_chunk, PIECES - 1)):
            relayed[i].wait_recv()
        forward(c)

    def partials(pair, side):
        start = pl.multiple_of(pair * 2 * strip, 2 * strip)
        decoder = both[1, pl.ds(start, 2 * strip), :]
        lo = pl.multiple_of(side * (QUADS * rows), QUADS * rows)
        value = lax.dot_general(
            act[pl.ds(lo, QUADS * rows), :], decoder, over_cols, preferred_element_type=f32
        ).astype(bf16)
        tail = lax.dot_general(
            hidden[...], decoder, over_cols, preferred_element_type=f32
        ).astype(bf16)
        for i in range(2):
            a, b = i * strip, (i + 1) * strip
            for j in range(QUADS):
                partial[pair * 2 + i, side * QUADS + j, 0:rows] = (
                    value[j * rows : (j + 1) * rows, a:b]
                )
                partial[pair * 2 + i, side * QUADS + j, rows:] = tail[:, a:b]

    def across(p):
        theirs = pl.ds(pl.multiple_of((1 - core) * QUADS, QUADS), QUADS)
        return remote(
            partial.at[p, theirs], first_in.at[p], s1.at[p], r1.at[p], *partner
        )

    def away(p, k):
        return remote(
            sums.at[p, k - 1], second_in.at[p, k - 1],
            s2.at[p * 3 + k - 1], r2.at[p * 3 + k - 1], *quad(k)[1],
        )

    def gather(p, k):
        if k == 0:
            return remote(
                misfit.at[p, mine], misfit.at[p, mine], s4.at[p * 4], r4.at[p * 4], *partner
            )
        return remote(
            misfit.at[p, mine], misfit.at[p, mine],
            s3.at[p * 3 + k - 1], r3.at[p * 3 + k - 1], *quad(k)[1],
        )

    def passing(p, k):
        came = misfit.at[p, core * QUADS + quad(k)[0]]
        return remote(came, came, s4.at[p * 4 + k], r4.at[p * 4 + k], *partner)

    def reduce_out(p):
        across(p).wait_recv()
        for k in (3, 1, 2):
            other = quad(k)[0]
            sums[p, k - 1] = (
                partial[p, core * QUADS + other].astype(f32) + first_in[p, other].astype(f32)
            ).astype(bf16)
            away(p, k).start()

    def compare(p):
        for k in range(1, QUADS):
            away(p, k).wait_recv()
        lanes = pl.ds(pl.multiple_of(p * strip, strip), strip)

        def whole(lo, hi):
            value = partial[p, mine, lo:hi].astype(f32) + first_in[p, q, lo:hi].astype(f32)
            for k in range(1, QUADS):
                value = value + second_in[p, k - 1, lo:hi].astype(f32)
            return value

        all_targets = targets[:, lanes].astype(f32)
        pool_row = lax.broadcasted_iota(jnp.int32, all_targets.shape, 0)
        tail_row = lax.broadcasted_iota(jnp.int32, (PAD, strip), 0)
        tail = jnp.zeros((PAD, strip), f32)
        outputs = whole(rows, rows + PAD)
        for i in range(spt):
            lo, hi = i * tangents, (i + 1) * tangents
            index = plan[0, sec * spt + i]
            misfit[p, mine, lo:hi] = (
                jacobian_weight * (whole(lo, hi) - jac[index, :, lanes].astype(f32))
            ).astype(bf16)
            target = jnp.sum(
                jnp.where(pool_row == index, all_targets, 0.0), axis=0, keepdims=True
            )
            tail = jnp.where(tail_row == mine * spt + i, outputs - target, tail)
        misfit[p, mine, rows:] = tail.astype(bf16)
        for k in (3, 1, 2, 0):
            gather(p, k).start()

    def pass_on(p):
        for k in (1, 2, 3):
            gather(p, k).wait_recv()
            passing(p, k).start()

    def last_of(p):
        for k in range(QUADS):
            (passing(p, k) if k else gather(p, 0)).wait_recv()
        lhs = jnp.concatenate([misfit[p, b, 0:rows] for b in range(2 * QUADS)], axis=0)
        value = lax.dot_general(lhs, act[...], over_rows, preferred_element_type=f32)
        tail = misfit[p, 0, rows:].astype(f32)
        for b in range(1, 2 * QUADS):
            tail = tail + misfit[p, b, rows:].astype(f32)
        value = value + lax.dot_general(
            tail.astype(bf16), hidden[...], over_rows, preferred_element_type=f32
        )
        here = pl.ds(pl.multiple_of(p * strip, strip), strip)
        last_total[here, :] = value
        last_grads[here, :] = value.astype(bf16)

    def slab_of(o):
        return pl.ds(pl.multiple_of(o * slab, slab), slab)

    def last_link(j, kind):
        here = slice(j * lw, (j + 1) * lw)
        if not line:
            o = others[kind]
            source = last_grads.at[slab_of(o), here]
        elif kind == 2:
            o, source = opposite, last_halves.at[:, here]
        else:
            o, source = mate, last_grads.at[slab_of([mate_opposite, mate][kind]), here]
        i = j * last_inbox.shape[0] + kind
        return remote(
            source, last_inbox.at[kind, :, here], s5.at[i], r5.at[i], o * GROUP + g, sec
        )

    def last_relay(j):
        last_link(j, 0).wait_recv()
        here = slice(j * lw, (j + 1) * lw)
        last_halves[:, here] = (
            last_total[slab_of(opposite), here] + last_inbox[0, :, here].astype(f32)
        ).astype(bf16)
        last_link(j, 2).start()

    def link(j, kind):
        if not line:
            o = others[kind]
            source = grads.at[j, slab_of(o), :]
        elif kind == 2:
            o, source = opposite, halves.at[j]
        else:
            o, source = mate, grads.at[j, slab_of([mate_opposite, mate][kind]), :]
        i = j * inbox.shape[1] + kind
        return remote(source, inbox.at[j, kind], s6.at[i], r6.at[i], o * GROUP + g, sec)

    def relay(j):
        link(j, 0).wait_recv()
        halves[j] = (
            total[j, slab_of(opposite), :] + inbox[j, 0].astype(f32)
        ).astype(bf16)
        link(j, 2).start()

    def columns(j):
        start = pl.multiple_of((sec * GROUP + g) * cols + j * zw, zw)
        return out.at[:, pl.ds(start, zw)]

    def hand(layer, j, k):
        h = lax.rem(g + k, GROUP)
        i = j * 2 * GROUP
        return remote(
            finished.at[layer, j, h], columns(j),
            s7.at[layer * LINKS * GROUP + j * GROUP + k], r7.at[i + sec * GROUP + k],
            base + h, layer,
        )

    kinds = range(1, 3) if line else range(n_s - 1)

    def finish(layer, j):
        for h in range(GROUP):
            start = pl.multiple_of(s * slab + h * own_rows, own_rows)
            here = slice(h * own_rows, (h + 1) * own_rows)
            if layer:
                lo, hi = j * zw, (j + 1) * zw
                value = last_total[pl.ds(start, own_rows), lo:hi]
                for k in kinds:
                    value = value + last_inbox[k, here, lo:hi].astype(f32)
            else:
                value = total[j, pl.ds(start, own_rows), :]
                for k in kinds:
                    value = value + inbox[j, k, here, :].astype(f32)
            finished[layer, j, h] = value.astype(bf16)
        for k in range(1, GROUP):
            hand(layer, j, k).start()

        @pl.when(sec != layer)
        def _():
            hand(layer, j, 0).start()

        @pl.when(sec == layer)
        def _():
            columns(j)[...] = finished[layer, j, g]

    def arrived(j):
        for k in kinds:
            link(j, k).wait_recv()

    def backward(j):
        lo, hi = j * cw, (j + 1) * cw

        def pull(i, carry):
            lhs = jnp.concatenate(
                [
                    jnp.concatenate(
                        [misfit[p, i * QUADS + b, 0:rows] for p in range(STRIPS)], axis=1
                    )
                    for b in range(QUADS)
                ],
                axis=0,
            )
            cot = jnp.dot(lhs, both[1, :, lo:hi], preferred_element_type=f32)
            start = pl.multiple_of(i * loop_rows, loop_rows)
            for t in range(loop_samples):
                part = cot[t * tangents : (t + 1) * tangents]
                here = pl.ds(pl.multiple_of(start + t * tangents, tangents), tangents)
                slope = first[pl.ds(i * loop_samples + t, 1), lo:hi]
                proj[pl.ds(i * loop_samples + t, 1), :] = jnp.sum(
                    part * picked[here, lo:hi].astype(f32), axis=0, keepdims=True
                )
                pulled[here, :] = (part * slope).astype(bf16)
            return carry

        lax.fori_loop(0, n_loop, pull, 0)
        tail = jnp.zeros((PAD, reduced), f32)
        for b in range(2 * QUADS):
            tail = tail + jnp.concatenate(
                [misfit[p, b, rows:] for p in range(STRIPS)], axis=1
            ).astype(f32)
        cot = jnp.dot(tail.astype(bf16), both[1, :, lo:hi], preferred_element_type=f32)
        pre = (cot * first[:, lo:hi] + second[:, lo:hi] * proj[...]).astype(bf16)
        value = jnp.dot(onehot[...], pulled[...], preferred_element_type=f32)
        value = value + lax.dot_general(
            xs[...].astype(bf16), pre, over_rows, preferred_element_type=f32
        )
        for i in range(cw // zw):
            total[j * (cw // zw) + i] = value[:, i * zw : (i + 1) * zw]
            grads[j * (cw // zw) + i] = value[:, i * zw : (i + 1) * zw].astype(bf16)

    def own_strip():
        lhs = jnp.concatenate(
            [misfit[order[3], b, 0:rows] for b in range(2 * QUADS)], axis=0
        )
        value = lax.dot_general(lhs, act[...], over_rows, preferred_element_type=f32)
        tail = misfit[order[3], 0, rows:].astype(f32)
        for b in range(1, 2 * QUADS):
            tail = tail + misfit[order[3], b, rows:].astype(f32)
        last_total[slab_of(s), :] = value + lax.dot_general(
            tail.astype(bf16), hidden[...], over_rows, preferred_element_type=f32
        )

    def onehots():
        for t in range(n_all):
            deep = lax.broadcasted_iota(jnp.int32, (reduced, tangents), 0).astype(f32)
            onehot[:, t * tangents : (t + 1) * tangents] = (
                (deep == dirs[t : t + 1, :]).astype(f32).astype(bf16)
            )

    for i in range(2):
        partials(pairs[i], 1 - core)
        across(order[2 * i]).start()
        across(order[2 * i + 1]).start()
        partials(pairs[i], core)
        if i == 0:
            reduce_out(order[0])
            reduce_out(order[1])
    onehots()
    load_jac.wait()
    compare(order[0])
    compare(order[1])
    reduce_out(order[2])
    reduce_out(order[3])
    pass_on(order[0])
    last_of(order[0])
    if line:
        for j in range(LASTS):
            last_link(j, 0).start()
    pass_on(order[1])
    last_of(order[1])
    compare(order[2])
    if line:
        last_relay(0)
    compare(order[3])
    if line:
        for j in range(1, LASTS):
            last_relay(j)
    pass_on(order[2])
    last_of(order[2])
    if line:
        for j in range(LASTS):
            last_link(j, 1).start()
    pass_on(order[3])
    if line:
        for k in range(QUADS):
            (passing(order[3], k) if k else gather(order[3], 0)).wait_recv()
        turns = [
            ([0, 1], [], []), ([2, 3], [], [0, 1]), ([4, 5], [0, 1], [2, 3]),
            ([6, 7], [2, 3], [4, 5]),
        ]
        for j, (out_first, through, out_second) in enumerate(turns):
            backward(j)
            for i in out_first:
                link(i, 0).start()
            for i in through:
                relay(i)
            for i in out_second:
                link(i, 1).start()
        own_strip()
        relay(4)
        relay(5)
        link(6, 1).start()
        link(7, 1).start()
        for i in range(LASTS):
            for k in kinds:
                last_link(i, k).wait_recv()
        for j in range(LINKS):
            finish(1, j)
        arrived(0)
        finish(0, 0)
        arrived(1)
        finish(0, 1)
        relay(6)
        relay(7)
        for j in range(2, LINKS):
            arrived(j)
            finish(0, j)
    else:
        last_of(order[3])
        for kind in range(n_s - 1):
            for j in range(LASTS):
                last_link(j, kind).start()
        for j in range(CHUNKS):
            backward(j)
            for kind in range(n_s - 1):
                for i in range(j * LINKS // CHUNKS, (j + 1) * LINKS // CHUNKS):
                    link(i, kind).start()
        for i in range(LASTS):
            for k in kinds:
                last_link(i, k).wait_recv()
        for j in range(LINKS):
            finish(1, j)
        for j in range(LINKS):
            arrived(j)
            finish(0, j)

    for copy in shared + sent + relayed:
        copy.wait_send()
    for p in range(STRIPS):
        across(p).wait_send()
        for k in range(1, QUADS):
            away(p, k).wait_send()
            passing(p, k).wait_send()
        for k in range(QUADS):
            gather(p, k).wait_send()
    for k in range(last_inbox.shape[0]):
        for j in range(LASTS):
            last_link(j, k).wait_send()
        for j in range(LINKS):
            link(j, k).wait_send()
    for layer in range(2):
        for j in range(LINKS):
            for k in range(1, GROUP):
                hand(layer, j, k).wait_send()

            @pl.when(sec != layer)
            def _():
                hand(layer, j, 0).wait_send()

    for j in range(LINKS):
        for i in range(2):
            for k in range(GROUP):
                at = j * 2 * GROUP + i * GROUP + k
                arrival = remote(
                    finished.at[0, j, 0], columns(j), s7.at[0], r7.at[at], *partner
                )
                if k:
                    arrival.wait_recv()
                else:

                    @pl.when(sec != i)
                    def _():
                        arrival.wait_recv()


def shards(n_dp, n_sec, samples, targets, jacobian_targets, directions, plan, weights):
    _, reduced, width = weights.shape
    pool, tangents = directions.shape
    team = n_sec * GROUP
    cols = width // team
    n_s = n_dp // GROUP
    spt = MICRO // n_sec
    rows = spt * tangents
    high = rows + PAD
    every = team * spt
    strip = reduced // STRIPS
    slab = reduced // n_s
    cw, zw = cols // CHUNKS, cols // LINKS
    kinds = 3 if n_s == 4 else n_s - 1
    f32, bf16 = jnp.float32, jnp.bfloat16
    vmem = pltpu.VMEM
    dma = lambda n: pltpu.SemaphoreType.DMA((n,))
    result = pl.pallas_call(
        functools.partial(fused_kernel, n_s),
        out_shape=jax.ShapeDtypeStruct((reduced // n_dp, width), bf16),
        in_specs=[pl.BlockSpec(memory_space=pltpu.SMEM), VMEM, VMEM, VMEM, ANY, ANY],
        out_specs=VMEM,
        scratch_shapes=[
            vmem((GROUP, pool, reduced + tangents), f32),
            vmem((n_sec, reduced, cols), bf16),
            vmem((reduced, cols), bf16),
            vmem(jacobian_targets.shape, bf16),
            vmem((every, reduced), f32),
            vmem((every, tangents), f32),
            vmem((every * tangents, reduced), bf16),
            vmem((reduced, every * tangents), bf16),
            vmem((every * tangents, cols), bf16),
            vmem((every, cols), bf16),
            vmem((every * tangents, cols), bf16),
            vmem((every, cols), f32),
            vmem((every, cols), f32),
            vmem((STRIPS, team, high, strip), bf16),
            vmem((STRIPS, QUADS, high, strip), bf16),
            vmem((STRIPS, QUADS - 1, high, strip), bf16),
            vmem((STRIPS, QUADS - 1, high, strip), bf16),
            vmem((STRIPS, team, high, strip), bf16),
            vmem((LINKS, reduced, zw), f32),
            vmem((LINKS, reduced, zw), bf16),
            vmem((LINKS, kinds, slab, zw), bf16),
            vmem((LINKS, slab, zw), bf16),
            vmem((reduced, cols), f32),
            vmem((reduced, cols), bf16),
            vmem((kinds, slab, cols), bf16),
            vmem((slab, cols), bf16),
            vmem((every * tangents, cw), bf16),
            vmem((every, cw), f32),
            vmem((n_sec, LINKS, GROUP, reduced // n_dp, zw), bf16),
            dma(GROUP - 1), dma(GROUP - 1), dma(PIECES + 1), dma(PIECES + 1),
            dma(PIECES - 1), dma(PIECES - 1),
            dma(STRIPS), dma(STRIPS), dma(STRIPS * 3), dma(STRIPS * 3),
            dma(STRIPS * 3), dma(STRIPS * 3), dma(STRIPS * 4), dma(STRIPS * 4),
            dma(LASTS * kinds), dma(LASTS * kinds), dma(LINKS * kinds), dma(LINKS * kinds),
            dma(2 * LINKS * GROUP), dma(2 * LINKS * GROUP), dma(3),
        ],
        compiler_params=pltpu.CompilerParams(
            collective_id=0, has_side_effects=True, vmem_limit_bytes=60 * 1024 * 1024
        ),
        name="fused",
    )(plan, samples, directions, targets, jacobian_targets, weights)
    return result.astype(f32)[None]


def solution(mesh):
    placed = (
        P("dp", None),
        P("dp", None),
        P("dp", None, None),
        P("dp", None),
        P("dp", None),
        P("section", None, None),
    )
    body = functools.partial(shards, mesh.shape["dp"], mesh.shape["section"])
    return jax.shard_map(
        body, mesh=mesh, in_specs=placed, out_specs=P("section", "dp", None), check_vma=False
    )
```

```python
import functools

import jax
import jax.numpy as jnp
from jax import lax
from jax.experimental import pallas as pl
from jax.experimental.pallas import tpu as pltpu
from jax.sharding import PartitionSpec as P

MICRO = 4
GROUP = 4
PAD = 16
PIECES = 8
CHUNKS = 4
STRIPS = 4
LINKS = 8
LASTS = 2
QUADS = 4

jacobian_weight = 32.0

VMEM = pl.BlockSpec(memory_space=pltpu.VMEM)
ANY = pl.BlockSpec(memory_space=pl.ANY)


def remote(src, dst, send, recv, dp, sec):
    return pltpu.make_async_remote_copy(
        src_ref=src, dst_ref=dst, send_sem=send, recv_sem=recv,
        device_id={"dp": dp, "section": sec},
    )


def fused_kernel(
    n_s, plan, samples, directions, targets, jac_hbm, weight, out,
    packs, both, mail, jac, xs, dirs, onehot_t, onehot, act, hidden, picked, first, second,
    partial, first_in, sums, second_in, misfit, total, grads, inbox, halves,
    last_total, last_grads, last_inbox, last_halves, pulled, proj, finished,
    psend, precv, wsend, wrecv, zsend, zrecv, s1, r1, s2, r2, s3, r3, s4, r4,
    s5, r5, s6, r6, s7, r7, local,
):
    f32, bf16 = jnp.float32, jnp.bfloat16
    dp, sec = lax.axis_index("dp"), lax.axis_index("section")
    g = lax.rem(dp, GROUP)
    base = dp - g
    s = dp // GROUP
    core, half = lax.rem(g, 2), g // 2
    q = sec * 2 + half
    mine = core * QUADS + q
    partner = (base + half * 2 + (1 - core), sec)
    parity = lax.rem(s, 2)
    mate = s + 1 - 2 * parity
    twin = (mate * GROUP + g, sec)
    line = n_s == 4
    reduced, cols = both.shape[1:]
    tangents = directions.shape[1]
    spt = MICRO // 2
    rows = spt * tangents
    strip = reduced // STRIPS
    slab = reduced // n_s
    own_rows = slab // GROUP
    cw = cols // CHUNKS
    pw = cols // PIECES
    zw = cols // LINKS
    lw = cols // LASTS
    over_rows = (((0,), (0,)), ((), ()))
    over_cols = (((1,), (1,)), ((), ()))

    def quad(k):
        l = 1 - sec if k & 2 else sec
        h = 1 - half if k & 1 else half
        return l * 2 + h, (base + h * 2 + core, l)

    if line:
        far_end, far_mid, across_z = 3 - 3 * (s // 2), 2 - s // 2, 3 - s
        middle = lax.rem(s + 1, 4) >= 2
        others = [mate]
        order = [far_end, far_mid, mate, s]
        pairs = [1 - s // 2, s // 2]
    else:
        others = [lax.rem(s + k, n_s) for k in range(1, n_s)]
        order = list(range(STRIPS))
        pairs = [0, 1]

    far_start = pl.multiple_of(((1 - sec) * GROUP + g) * cols, cols)
    load_mail = pltpu.make_async_copy(
        weight.at[0, :, pl.ds(far_start, cols)], mail, local.at[2]
    )
    load_mail.start()
    own = pltpu.make_async_copy(
        weight.at[0, :, pl.ds(pl.multiple_of((sec * GROUP + g) * cols, cols), cols)],
        both.at[sec], local.at[0],
    )
    own.start()
    load_jac = pltpu.make_async_copy(jac_hbm, jac, local.at[1])
    load_jac.start()

    barrier = pltpu.get_barrier_semaphore()
    peers = [
        (base + lax.rem(g + k, GROUP), 1 - sec if j else sec)
        for j in range(2) for k in range(GROUP) if j or k
    ] + [(o * GROUP + g, sec) for o in others]
    for d, l in peers:
        pl.semaphore_signal(barrier, inc=1, device_id={"dp": d, "section": l})
    if line:

        @pl.when(middle)
        def _():
            pl.semaphore_signal(
                barrier, inc=1, device_id={"dp": across_z * GROUP + g, "section": sec}
            )

    pl.semaphore_wait(barrier, len(peers) + (jnp.where(middle, 1, 0) if line else 0))


    side = reduced // 2
    half_rows = pl.ds(pl.multiple_of(parity * side, side), side)
    other_rows = pl.ds(pl.multiple_of((1 - parity) * side, side), side)
    load_mail.wait()
    sent, relayed = [], []
    for c in range(PIECES + 1):
        here = (half_rows if c < PIECES else other_rows, pl.ds(min(c, PIECES - 1) * pw, pw))
        sent.append(remote(
            mail.at[here], both.at[(sec,) + here], wsend.at[c], wrecv.at[c], dp, 1 - sec,
        ))
        sent[-1].start()

    every = jnp.concatenate(
        [samples[...].astype(f32), directions[...].astype(f32)], axis=1
    )
    row = lax.broadcasted_iota(jnp.int32, every.shape, 0)
    packed = jnp.zeros_like(every)
    for k in range(MICRO):
        chosen = jnp.sum(jnp.where(row == plan[0, k], every, 0.0), axis=0, keepdims=True)
        packed = jnp.where(row == k, chosen, packed)
    packs[g] = packed
    shared = []
    for k in range(1, GROUP):
        shared.append(remote(
            packs.at[g], packs.at[g], psend.at[k - 1], precv.at[k - 1],
            base + lax.rem(g + k, GROUP), sec,
        ))
        shared[-1].start()

    def arrive(c):
        sent[c].wait_recv()
        if c < PIECES - 1:
            came = both.at[1 - sec, half_rows, pl.ds(c * pw, pw)]
            relayed.append(remote(came, came, zsend.at[c], zrecv.at[c], *twin))
            relayed[-1].start()

    arrive(0)
    for copy in shared:
        copy.wait_recv()
    for b in range(2 * QUADS):
        c, l, h = b // QUADS, (b % QUADS) // 2, b % 2
        xs[b * spt : (b + 1) * spt] = packs[h * 2 + c, l * spt : (l + 1) * spt, :reduced]
        dirs[b * spt : (b + 1) * spt] = packs[h * 2 + c, l * spt : (l + 1) * spt, reduced:]
    n_all = 2 * QUADS * spt
    turned = dirs[...].T

    def spread_directions(ts):
        for t in ts:
            lane = lax.broadcasted_iota(jnp.int32, (tangents, reduced), 1).astype(f32)
            onehot_t[t * tangents : (t + 1) * tangents] = (
                (lane == turned[:, t : t + 1]).astype(f32).astype(bf16)
            )

    arrive(1)
    spread_directions(range(n_all // 2))
    arrive(2)
    spread_directions(range(n_all // 2, n_all))
    arrive(3)

    n_loop = 2
    loop_rows = n_all * tangents // n_loop
    loop_samples = n_all // n_loop

    def forward(c):
        lo, hi = c * cw, (c + 1) * cw
        linear = jnp.dot(xs[...].astype(bf16), both[0, :, lo:hi], preferred_element_type=f32)
        squash = jax.nn.sigmoid(linear)
        first[:, lo:hi] = squash * (1.0 + linear * (1.0 - squash))
        second[:, lo:hi] = squash * (1.0 - squash) * (2.0 + linear * (1.0 - 2.0 * squash))
        hidden[:, lo:hi] = (linear * squash).astype(bf16)

        def pick(i, carry):
            start = pl.multiple_of(i * loop_rows, loop_rows)
            value = jnp.dot(
                onehot_t[pl.ds(start, loop_rows), :], both[0, :, lo:hi],
                preferred_element_type=f32,
            )
            picked[pl.ds(start, loop_rows), lo:hi] = value.astype(bf16)
            for t in range(loop_samples):
                slope = first[pl.ds(i * loop_samples + t, 1), lo:hi]
                here = pl.ds(pl.multiple_of(start + t * tangents, tangents), tangents)
                act[here, lo:hi] = (
                    slope * value[t * tangents : (t + 1) * tangents]
                ).astype(bf16)
            return carry

        lax.fori_loop(0, n_loop, pick, 0)

    own.wait()
    per_chunk = PIECES // CHUNKS
    for c in range(CHUNKS):
        for i in ([], [4, 5], [6], [7, 8])[c]:
            arrive(i)
        for i in range(c * per_chunk, min((c + 1) * per_chunk, PIECES - 1)):
            relayed[i].wait_recv()
        forward(c)

    def partials(pair, side):
        start = pl.multiple_of(pair * 2 * strip, 2 * strip)
        decoder = both[1, pl.ds(start, 2 * strip), :]
        lo = pl.multiple_of(side * (QUADS * rows), QUADS * rows)
        value = lax.dot_general(
            act[pl.ds(lo, QUADS * rows), :], decoder, over_cols, preferred_element_type=f32
        ).astype(bf16)
        tail = lax.dot_general(
            hidden[...], decoder, over_cols, preferred_element_type=f32
        ).astype(bf16)
        for i in range(2):
            a, b = i * strip, (i + 1) * strip
            for j in range(QUADS):
                partial[pair * 2 + i, side * QUADS + j, 0:rows] = (
                    value[j * rows : (j + 1) * rows, a:b]
                )
                partial[pair * 2 + i, side * QUADS + j, rows:] = tail[:, a:b]

    def across(p):
        theirs = pl.ds(pl.multiple_of((1 - core) * QUADS, QUADS), QUADS)
        return remote(
            partial.at[p, theirs], first_in.at[p], s1.at[p], r1.at[p], *partner
        )

    def away(p, k):
        return remote(
            sums.at[p, k - 1], second_in.at[p, k - 1],
            s2.at[p * 3 + k - 1], r2.at[p * 3 + k - 1], *quad(k)[1],
        )

    def gather(p, k):
        if k == 0:
            return remote(
                misfit.at[p, mine], misfit.at[p, mine], s4.at[p * 4], r4.at[p * 4], *partner
            )
        return remote(
            misfit.at[p, mine], misfit.at[p, mine],
            s3.at[p * 3 + k - 1], r3.at[p * 3 + k - 1], *quad(k)[1],
        )

    def passing(p, k):
        came = misfit.at[p, core * QUADS + quad(k)[0]]
        return remote(came, came, s4.at[p * 4 + k], r4.at[p * 4 + k], *partner)

    def reduce_out(p):
        across(p).wait_recv()
        for k in (3, 1, 2):
            other = quad(k)[0]
            sums[p, k - 1] = (
                partial[p, core * QUADS + other].astype(f32) + first_in[p, other].astype(f32)
            ).astype(bf16)
            away(p, k).start()

    def compare(p):
        for k in range(1, QUADS):
            away(p, k).wait_recv()
        lanes = pl.ds(pl.multiple_of(p * strip, strip), strip)

        def whole(lo, hi):
            value = partial[p, mine, lo:hi].astype(f32) + first_in[p, q, lo:hi].astype(f32)
            for k in range(1, QUADS):
                value = value + second_in[p, k - 1, lo:hi].astype(f32)
            return value

        all_targets = targets[:, lanes].astype(f32)
        pool_row = lax.broadcasted_iota(jnp.int32, all_targets.shape, 0)
        tail_row = lax.broadcasted_iota(jnp.int32, (PAD, strip), 0)
        tail = jnp.zeros((PAD, strip), f32)
        outputs = whole(rows, rows + PAD)
        for i in range(spt):
            lo, hi = i * tangents, (i + 1) * tangents
            index = plan[0, sec * spt + i]
            misfit[p, mine, lo:hi] = (
                jacobian_weight * (whole(lo, hi) - jac[index, :, lanes].astype(f32))
            ).astype(bf16)
            target = jnp.sum(
                jnp.where(pool_row == index, all_targets, 0.0), axis=0, keepdims=True
            )
            tail = jnp.where(tail_row == mine * spt + i, outputs - target, tail)
        misfit[p, mine, rows:] = tail.astype(bf16)
        for k in (3, 1, 2, 0):
            gather(p, k).start()

    def pass_on(p):
        for k in (1, 2, 3):
            gather(p, k).wait_recv()
            passing(p, k).start()

    def last_of(p):
        for k in range(QUADS):
            (passing(p, k) if k else gather(p, 0)).wait_recv()
        lhs = jnp.concatenate([misfit[p, b, 0:rows] for b in range(2 * QUADS)], axis=0)
        value = lax.dot_general(lhs, act[...], over_rows, preferred_element_type=f32)
        tail = misfit[p, 0, rows:].astype(f32)
        for b in range(1, 2 * QUADS):
            tail = tail + misfit[p, b, rows:].astype(f32)
        value = value + lax.dot_general(
            tail.astype(bf16), hidden[...], over_rows, preferred_element_type=f32
        )
        here = pl.ds(pl.multiple_of(p * strip, strip), strip)
        last_total[here, :] = value
        last_grads[here, :] = value.astype(bf16)

    def slab_of(o):
        return pl.ds(pl.multiple_of(o * slab, slab), slab)

    def last_link(j, kind, source=None, o=None):
        here = slice(j * lw, (j + 1) * lw)
        if source is None:
            o = others[kind] if not line else mate
            slab_at = o if not line else order[min(kind, 2)]
            source = last_grads.at[slab_of(slab_at), here]
        i = j * last_inbox.shape[0] + kind
        return remote(
            source, last_inbox.at[kind, :, here], s5.at[i], r5.at[i], o * GROUP + g, sec
        )

    def link(j, kind, source=None, o=None):
        if source is None:
            o = others[kind] if not line else mate
            slab_at = o if not line else order[min(kind, 2)]
            source = grads.at[j, slab_of(slab_at), :]
        i = j * inbox.shape[1] + kind
        return remote(source, inbox.at[j, kind], s6.at[i], r6.at[i], o * GROUP + g, sec)

    if line:
        turns = [(0, far_end, 3, across_z), (1, far_mid, 4, across_z), (3, mate, 2, mate)]

    def last_onward(j, r):
        return last_link(
            j, turns[r][2], last_halves.at[r, :, slice(j * lw, (j + 1) * lw)], turns[r][3]
        )

    def last_relay(j, r):
        @pl.when(middle)
        def _():
            kind, o, _, _ = turns[r]
            here = slice(j * lw, (j + 1) * lw)
            last_link(j, kind).wait_recv()
            last_halves[r, :, here] = (
                last_total[slab_of(o), here] + last_inbox[kind, :, here].astype(f32)
            ).astype(bf16)
            last_onward(j, r).start()

    def onward(j, r):
        return link(j, turns[r][2], halves.at[j, r], turns[r][3])

    def relay(j, r):
        @pl.when(middle)
        def _():
            kind, o, _, _ = turns[r]
            link(j, kind).wait_recv()
            halves[j, r] = (
                total[j, slab_of(o), :] + inbox[j, kind].astype(f32)
            ).astype(bf16)
            onward(j, r).start()

    def from_end(copies):
        @pl.when(jnp.logical_not(middle))
        def _():
            for copy in copies:
                copy.start()

    def columns(j):
        start = pl.multiple_of((sec * GROUP + g) * cols + j * zw, zw)
        return out.at[:, pl.ds(start, zw)]

    def hand(layer, j, k):
        h = lax.rem(g + k, GROUP)
        i = j * 2 * GROUP
        return remote(
            finished.at[layer, j, h], columns(j),
            s7.at[layer * LINKS * GROUP + j * GROUP + k], r7.at[i + sec * GROUP + k],
            base + h, layer,
        )

    def add_up(layer, j, kinds):
        for h in range(GROUP):
            start = pl.multiple_of(s * slab + h * own_rows, own_rows)
            here = slice(h * own_rows, (h + 1) * own_rows)
            if layer:
                lo, hi = j * zw, (j + 1) * zw
                value = last_total[pl.ds(start, own_rows), lo:hi]
                for k in kinds:
                    value = value + last_inbox[k, here, lo:hi].astype(f32)
            else:
                value = total[j, pl.ds(start, own_rows), :]
                for k in kinds:
                    value = value + inbox[j, k, here, :].astype(f32)
            finished[layer, j, h] = value.astype(bf16)

    def finish(layer, j):
        if line:

            @pl.when(middle)
            def _():
                add_up(layer, j, (2, 4))

            @pl.when(jnp.logical_not(middle))
            def _():
                add_up(layer, j, (2,))
        else:
            add_up(layer, j, range(n_s - 1))
        for k in range(1, GROUP):
            hand(layer, j, k).start()

        @pl.when(sec != layer)
        def _():
            hand(layer, j, 0).start()

        @pl.when(sec == layer)
        def _():
            columns(j)[...] = finished[layer, j, g]

    def landed(j, one):
        if line:
            one(j, 2).wait_recv()

            @pl.when(middle)
            def _():
                one(j, 4).wait_recv()
        else:
            for k in range(n_s - 1):
                one(j, k).wait_recv()

    def arrived(j):
        landed(j, link)

    def backward(j):
        lo, hi = j * cw, (j + 1) * cw

        def pull(i, carry):
            lhs = jnp.concatenate(
                [
                    jnp.concatenate(
                        [misfit[p, i * QUADS + b, 0:rows] for p in range(STRIPS)], axis=1
                    )
                    for b in range(QUADS)
                ],
                axis=0,
            )
            cot = jnp.dot(lhs, both[1, :, lo:hi], preferred_element_type=f32)
            start = pl.multiple_of(i * loop_rows, loop_rows)
            for t in range(loop_samples):
                part = cot[t * tangents : (t + 1) * tangents]
                here = pl.ds(pl.multiple_of(start + t * tangents, tangents), tangents)
                slope = first[pl.ds(i * loop_samples + t, 1), lo:hi]
                proj[pl.ds(i * loop_samples + t, 1), :] = jnp.sum(
                    part * picked[here, lo:hi].astype(f32), axis=0, keepdims=True
                )
                pulled[here, :] = (part * slope).astype(bf16)
            return carry

        lax.fori_loop(0, n_loop, pull, 0)
        tail = jnp.zeros((PAD, reduced), f32)
        for b in range(2 * QUADS):
            tail = tail + jnp.concatenate(
                [misfit[p, b, rows:] for p in range(STRIPS)], axis=1
            ).astype(f32)
        cot = jnp.dot(tail.astype(bf16), both[1, :, lo:hi], preferred_element_type=f32)
        pre = (cot * first[:, lo:hi] + second[:, lo:hi] * proj[...]).astype(bf16)
        value = jnp.dot(onehot[...], pulled[...], preferred_element_type=f32)
        value = value + lax.dot_general(
            xs[...].astype(bf16), pre, over_rows, preferred_element_type=f32
        )
        for i in range(cw // zw):
            total[j * (cw // zw) + i] = value[:, i * zw : (i + 1) * zw]
            grads[j * (cw // zw) + i] = value[:, i * zw : (i + 1) * zw].astype(bf16)

    def own_strip():
        lhs = jnp.concatenate(
            [misfit[order[3], b, 0:rows] for b in range(2 * QUADS)], axis=0
        )
        value = lax.dot_general(lhs, act[...], over_rows, preferred_element_type=f32)
        tail = misfit[order[3], 0, rows:].astype(f32)
        for b in range(1, 2 * QUADS):
            tail = tail + misfit[order[3], b, rows:].astype(f32)
        last_total[slab_of(s), :] = value + lax.dot_general(
            tail.astype(bf16), hidden[...], over_rows, preferred_element_type=f32
        )

    def onehots():
        for t in range(n_all):
            deep = lax.broadcasted_iota(jnp.int32, (reduced, tangents), 0).astype(f32)
            onehot[:, t * tangents : (t + 1) * tangents] = (
                (deep == dirs[t : t + 1, :]).astype(f32).astype(bf16)
            )

    for i in range(2):
        partials(pairs[i], 1 - core)
        across(order[2 * i]).start()
        across(order[2 * i + 1]).start()
        partials(pairs[i], core)
        if i == 0:
            reduce_out(order[0])
            reduce_out(order[1])
    onehots()
    load_jac.wait()
    compare(order[0])
    compare(order[1])
    reduce_out(order[2])
    reduce_out(order[3])
    pass_on(order[0])
    last_of(order[0])
    if line:
        from_end([last_link(j, 0) for j in range(LASTS)])
    pass_on(order[1])
    last_of(order[1])
    if line:
        from_end([last_link(j, 1) for j in range(LASTS)])
    compare(order[2])
    if line:
        last_relay(0, 0)
    compare(order[3])
    if line:
        for j in range(1, LASTS):
            last_relay(j, 0)
    pass_on(order[2])
    last_of(order[2])
    if line:
        from_end([last_link(j, 2) for j in range(LASTS)])
    pass_on(order[3])
    per_chunk = LINKS // CHUNKS
    if line:
        last_relay(0, 1)
        for k in range(QUADS):
            (passing(order[3], k) if k else gather(order[3], 0)).wait_recv()
        last_relay(0, 2)
        for j in range(CHUNKS):
            backward(j)
            pieces = range(j * per_chunk, (j + 1) * per_chunk)
            from_end([link(i, k) for k in range(2) for i in pieces])
            if j == 0:
                for i in range(1, LASTS):
                    last_relay(i, 1)
                    last_relay(i, 2)
            if j == 2:
                for r in range(2):
                    for i in range(2):
                        relay(i, r)
        from_end([link(i, 2) for i in range(LINKS)])
        def pass_along(*pieces):
            for r in range(2):
                for i in pieces:
                    relay(i, r)

        def bring_back(*pieces):
            for i in pieces:
                relay(i, 2)

        pass_along(2, 3)
        bring_back(0, 1)
        own_strip()
        pass_along(4, 5)
        bring_back(2, 3)
        for i in range(LASTS):
            landed(i, last_link)
        for j in range(LINKS):
            finish(1, j)
        pass_along(6)
        bring_back(4)
        pass_along(7)
        bring_back(5, 6, 7)
        for j in range(LINKS):
            arrived(j)
            finish(0, j)
    else:
        last_of(order[3])
        for kind in range(n_s - 1):
            for j in range(LASTS):
                last_link(j, kind).start()
        for j in range(CHUNKS):
            backward(j)
            for kind in range(n_s - 1):
                for i in range(j * per_chunk, (j + 1) * per_chunk):
                    link(i, kind).start()
        for i in range(LASTS):
            landed(i, last_link)
        for j in range(LINKS):
            finish(1, j)
        for j in range(LINKS):
            arrived(j)
            finish(0, j)

    for copy in shared + sent + relayed:
        copy.wait_send()
    for p in range(STRIPS):
        across(p).wait_send()
        for k in range(1, QUADS):
            away(p, k).wait_send()
            passing(p, k).wait_send()
        for k in range(QUADS):
            gather(p, k).wait_send()
    if line:

        @pl.when(middle)
        def _():
            for r in range(3):
                for j in range(LASTS):
                    last_onward(j, r).wait_send()
                for j in range(LINKS):
                    onward(j, r).wait_send()

        @pl.when(jnp.logical_not(middle))
        def _():
            for k in range(3):
                for j in range(LASTS):
                    last_link(j, k).wait_send()
                for j in range(LINKS):
                    link(j, k).wait_send()
    else:
        for k in range(n_s - 1):
            for j in range(LASTS):
                last_link(j, k).wait_send()
            for j in range(LINKS):
                link(j, k).wait_send()
    for layer in range(2):
        for j in range(LINKS):
            for k in range(1, GROUP):
                hand(layer, j, k).wait_send()

            @pl.when(sec != layer)
            def _():
                hand(layer, j, 0).wait_send()

    for j in range(LINKS):
        for i in range(2):
            for k in range(GROUP):
                at = j * 2 * GROUP + i * GROUP + k
                arrival = remote(
                    finished.at[0, j, 0], columns(j), s7.at[0], r7.at[at], *partner
                )
                if k:
                    arrival.wait_recv()
                else:

                    @pl.when(sec != i)
                    def _():
                        arrival.wait_recv()


def shards(n_dp, n_sec, samples, targets, jacobian_targets, directions, plan, weights):
    _, reduced, width = weights.shape
    pool, tangents = directions.shape
    team = n_sec * GROUP
    cols = width // team
    n_s = n_dp // GROUP
    spt = MICRO // n_sec
    rows = spt * tangents
    high = rows + PAD
    every = team * spt
    strip = reduced // STRIPS
    slab = reduced // n_s
    cw, zw = cols // CHUNKS, cols // LINKS
    kinds = 5 if n_s == 4 else n_s - 1
    f32, bf16 = jnp.float32, jnp.bfloat16
    vmem = pltpu.VMEM
    dma = lambda n: pltpu.SemaphoreType.DMA((n,))
    result = pl.pallas_call(
        functools.partial(fused_kernel, n_s),
        out_shape=jax.ShapeDtypeStruct((reduced // n_dp, width), bf16),
        in_specs=[pl.BlockSpec(memory_space=pltpu.SMEM), VMEM, VMEM, VMEM, ANY, ANY],
        out_specs=VMEM,
        scratch_shapes=[
            vmem((GROUP, pool, reduced + tangents), f32),
            vmem((n_sec, reduced, cols), bf16),
            vmem((reduced, cols), bf16),
            vmem(jacobian_targets.shape, bf16),
            vmem((every, reduced), f32),
            vmem((every, tangents), f32),
            vmem((every * tangents, reduced), bf16),
            vmem((reduced, every * tangents), bf16),
            vmem((every * tangents, cols), bf16),
            vmem((every, cols), bf16),
            vmem((every * tangents, cols), bf16),
            vmem((every, cols), f32),
            vmem((every, cols), f32),
            vmem((STRIPS, team, high, strip), bf16),
            vmem((STRIPS, QUADS, high, strip), bf16),
            vmem((STRIPS, QUADS - 1, high, strip), bf16),
            vmem((STRIPS, QUADS - 1, high, strip), bf16),
            vmem((STRIPS, team, high, strip), bf16),
            vmem((LINKS, reduced, zw), f32),
            vmem((LINKS, reduced, zw), bf16),
            vmem((LINKS, kinds, slab, zw), bf16),
            vmem((LINKS, 3, slab, zw), bf16),
            vmem((reduced, cols), f32),
            vmem((reduced, cols), bf16),
            vmem((kinds, slab, cols), bf16),
            vmem((3, slab, cols), bf16),
            vmem((every * tangents, cw), bf16),
            vmem((every, cw), f32),
            vmem((n_sec, LINKS, GROUP, reduced // n_dp, zw), bf16),
            dma(GROUP - 1), dma(GROUP - 1), dma(PIECES + 1), dma(PIECES + 1),
            dma(PIECES - 1), dma(PIECES - 1),
            dma(STRIPS), dma(STRIPS), dma(STRIPS * 3), dma(STRIPS * 3),
            dma(STRIPS * 3), dma(STRIPS * 3), dma(STRIPS * 4), dma(STRIPS * 4),
            dma(LASTS * kinds), dma(LASTS * kinds), dma(LINKS * kinds), dma(LINKS * kinds),
            dma(2 * LINKS * GROUP), dma(2 * LINKS * GROUP), dma(3),
        ],
        compiler_params=pltpu.CompilerParams(
            collective_id=0, has_side_effects=True, vmem_limit_bytes=60 * 1024 * 1024
        ),
        name="fused",
    )(plan, samples, directions, targets, jacobian_targets, weights)
    return result.astype(f32)[None]


def solution(mesh):
    placed = (
        P("dp", None),
        P("dp", None),
        P("dp", None, None),
        P("dp", None),
        P("dp", None),
        P("section", None, None),
    )
    body = functools.partial(shards, mesh.shape["dp"], mesh.shape["section"])
    return jax.shard_map(
        body, mesh=mesh, in_specs=placed, out_specs=P("section", "dp", None), check_vma=False
    )
```

```python
import functools

import jax
import jax.numpy as jnp
from jax import lax
from jax.experimental import pallas as pl
from jax.experimental.pallas import tpu as pltpu
from jax.sharding import PartitionSpec as P

MICRO = 4
GROUP = 4
PAD = 16
PIECES = 8
CHUNKS = 4
STRIPS = 4
LINKS = 8
LASTS = 2
QUADS = 4

jacobian_weight = 32.0

ANY = pl.BlockSpec(memory_space=pl.ANY)


def remote(src, dst, send, recv, dp, sec):
    return pltpu.make_async_remote_copy(
        src_ref=src, dst_ref=dst, send_sem=send, recv_sem=recv,
        device_id={"dp": dp, "section": sec},
    )


def fused_kernel(
    n_s, plan, samples_hbm, directions_hbm, targets_hbm, jac_hbm, weight, out,
    samples, directions, targets, packs, both, mail, jac, xs, dirs, onehot_t, onehot, act, hidden, picked, first, second,
    partial, first_in, sums, second_in, misfit, total, grads, inbox, halves,
    last_total, last_grads, last_inbox, last_halves, pulled, proj, finished,
    psend, precv, wsend, wrecv, zsend, zrecv, s1, r1, s2, r2, s3, r3, s4, r4,
    s5, r5, s6, r6, s7, r7, local,
):
    f32, bf16 = jnp.float32, jnp.bfloat16
    dp, sec = lax.axis_index("dp"), lax.axis_index("section")
    g = lax.rem(dp, GROUP)
    base = dp - g
    s = dp // GROUP
    core, half = lax.rem(g, 2), g // 2
    q = sec * 2 + half
    mine = core * QUADS + q
    partner = (base + half * 2 + (1 - core), sec)
    parity = lax.rem(s, 2)
    mate = s + 1 - 2 * parity
    twin = (mate * GROUP + g, sec)
    line = n_s == 4
    reduced, cols = both.shape[1:]
    tangents = directions.shape[1]
    spt = MICRO // 2
    rows = spt * tangents
    strip = reduced // STRIPS
    slab = reduced // n_s
    own_rows = slab // GROUP
    cw = cols // CHUNKS
    pw = cols // PIECES
    zw = cols // LINKS
    lw = cols // LASTS
    over_rows = (((0,), (0,)), ((), ()))
    over_cols = (((1,), (1,)), ((), ()))

    def quad(k):
        l = 1 - sec if k & 2 else sec
        h = 1 - half if k & 1 else half
        return l * 2 + h, (base + h * 2 + core, l)

    if line:
        far_end, far_mid, across_z = 3 - 3 * (s // 2), 2 - s // 2, 3 - s
        middle = lax.rem(s + 1, 4) >= 2
        others = [mate]
        order = [far_end, far_mid, mate, s]
        pairs = [1 - s // 2, s // 2]
    else:
        others = [lax.rem(s + k, n_s) for k in range(1, n_s)]
        order = list(range(STRIPS))
        pairs = [0, 1]

    far_start = pl.multiple_of(((1 - sec) * GROUP + g) * cols, cols)
    load_mail = pltpu.make_async_copy(
        weight.at[0, :, pl.ds(far_start, cols)], mail, local.at[2]
    )
    load_mail.start()
    own = pltpu.make_async_copy(
        weight.at[0, :, pl.ds(pl.multiple_of((sec * GROUP + g) * cols, cols), cols)],
        both.at[sec], local.at[0],
    )
    own.start()
    load_jac = pltpu.make_async_copy(jac_hbm, jac, local.at[1])
    load_jac.start()
    loads = [
        pltpu.make_async_copy(a, b, local.at[4 + i])
        for i, (a, b) in enumerate(
            ((samples_hbm, samples), (directions_hbm, directions), (targets_hbm, targets))
        )
    ]
    for copy in loads:
        copy.start()

    barrier = pltpu.get_barrier_semaphore()
    peers = [
        (base + lax.rem(g + k, GROUP), 1 - sec if j else sec)
        for j in range(2) for k in range(GROUP) if j or k
    ] + [(o * GROUP + g, sec) for o in others]
    for d, l in peers:
        pl.semaphore_signal(barrier, inc=1, device_id={"dp": d, "section": l})
    if line:

        @pl.when(middle)
        def _():
            pl.semaphore_signal(
                barrier, inc=1, device_id={"dp": across_z * GROUP + g, "section": sec}
            )

    pl.semaphore_wait(barrier, len(peers) + (jnp.where(middle, 1, 0) if line else 0))


    side = reduced // 2
    half_rows = pl.ds(pl.multiple_of(parity * side, side), side)
    other_rows = pl.ds(pl.multiple_of((1 - parity) * side, side), side)
    load_mail.wait()
    sent, relayed = [], []
    for c in range(PIECES + 1):
        here = (half_rows if c < PIECES else other_rows, pl.ds(min(c, PIECES - 1) * pw, pw))
        sent.append(remote(
            mail.at[here], both.at[(sec,) + here], wsend, wrecv.at[c], dp, 1 - sec,
        ))
        sent[-1].start()

    for copy in loads:
        copy.wait()
    every = jnp.concatenate(
        [samples[...].astype(f32), directions[...].astype(f32)], axis=1
    )
    row = lax.broadcasted_iota(jnp.int32, every.shape, 0)
    packed = jnp.zeros_like(every)
    for k in range(MICRO):
        chosen = jnp.sum(jnp.where(row == plan[0, k], every, 0.0), axis=0, keepdims=True)
        packed = jnp.where(row == k, chosen, packed)
    packs[g] = packed
    shared = []
    for k in range(1, GROUP):
        shared.append(remote(
            packs.at[g], packs.at[g], psend, precv,
            base + lax.rem(g + k, GROUP), sec,
        ))
        shared[-1].start()

    def arrive(c):
        sent[c].wait_recv()
        if c < PIECES - 1:
            came = both.at[1 - sec, half_rows, pl.ds(c * pw, pw)]
            relayed.append(remote(came, came, zsend, zrecv.at[c], *twin))
            relayed[-1].start()

    arrive(0)
    several = packs.at[0 : GROUP - 1]
    remote(several, several, psend, precv, *partner).wait_recv()
    for b in range(2 * QUADS):
        c, l, h = b // QUADS, (b % QUADS) // 2, b % 2
        xs[b * spt : (b + 1) * spt] = packs[h * 2 + c, l * spt : (l + 1) * spt, :reduced]
        dirs[b * spt : (b + 1) * spt] = packs[h * 2 + c, l * spt : (l + 1) * spt, reduced:]
    n_all = 2 * QUADS * spt
    turned = dirs[...].T

    def spread_directions(ts):
        for t in ts:
            lane = lax.broadcasted_iota(jnp.int32, (tangents, reduced), 1).astype(f32)
            onehot_t[t * tangents : (t + 1) * tangents] = (
                (lane == turned[:, t : t + 1]).astype(f32).astype(bf16)
            )

    arrive(1)
    spread_directions(range(n_all // 2))
    arrive(2)
    spread_directions(range(n_all // 2, n_all))
    arrive(3)

    n_loop = 2
    loop_rows = n_all * tangents // n_loop
    loop_samples = n_all // n_loop

    def forward(c):
        lo, hi = c * cw, (c + 1) * cw
        linear = jnp.dot(xs[...].astype(bf16), both[0, :, lo:hi], preferred_element_type=f32)
        squash = jax.nn.sigmoid(linear)
        first[:, lo:hi] = squash * (1.0 + linear * (1.0 - squash))
        second[:, lo:hi] = squash * (1.0 - squash) * (2.0 + linear * (1.0 - 2.0 * squash))
        hidden[:, lo:hi] = (linear * squash).astype(bf16)

        def pick(i, carry):
            start = pl.multiple_of(i * loop_rows, loop_rows)
            value = jnp.dot(
                onehot_t[pl.ds(start, loop_rows), :], both[0, :, lo:hi],
                preferred_element_type=f32,
            )
            picked[pl.ds(start, loop_rows), lo:hi] = value.astype(bf16)
            for t in range(loop_samples):
                slope = first[pl.ds(i * loop_samples + t, 1), lo:hi]
                here = pl.ds(pl.multiple_of(start + t * tangents, tangents), tangents)
                act[here, lo:hi] = (
                    slope * value[t * tangents : (t + 1) * tangents]
                ).astype(bf16)
            return carry

        lax.fori_loop(0, n_loop, pick, 0)

    own.wait()
    per_chunk = PIECES // CHUNKS
    for c in range(CHUNKS):
        for i in ([], [4, 5], [6], [7, 8])[c]:
            arrive(i)
        for i in range(c * per_chunk, min((c + 1) * per_chunk, PIECES - 1)):
            relayed[i].wait_recv()
        forward(c)

    def partials(pair, side):
        start = pl.multiple_of(pair * 2 * strip, 2 * strip)
        decoder = both[1, pl.ds(start, 2 * strip), :]
        lo = pl.multiple_of(side * (QUADS * rows), QUADS * rows)
        value = lax.dot_general(
            act[pl.ds(lo, QUADS * rows), :], decoder, over_cols, preferred_element_type=f32
        ).astype(bf16)
        tail = lax.dot_general(
            hidden[...], decoder, over_cols, preferred_element_type=f32
        ).astype(bf16)
        for i in range(2):
            a, b = i * strip, (i + 1) * strip
            for j in range(QUADS):
                partial[pair * 2 + i, side * QUADS + j, 0:rows] = (
                    value[j * rows : (j + 1) * rows, a:b]
                )
                partial[pair * 2 + i, side * QUADS + j, rows:] = tail[:, a:b]

    def across(p):
        theirs = pl.ds(pl.multiple_of((1 - core) * QUADS, QUADS), QUADS)
        return remote(
            partial.at[p, theirs], first_in.at[p], s1, r1.at[p], *partner
        )

    def away(p, k):
        return remote(
            sums.at[p, k - 1], second_in.at[p, k - 1],
            s2, r2.at[p], *quad(k)[1],
        )

    def gather(p, k):
        if k == 0:
            return remote(
                misfit.at[p, mine], misfit.at[p, mine], s4, r4.at[p], *partner
            )
        return remote(
            misfit.at[p, mine], misfit.at[p, mine],
            s3, r3.at[p * 3 + k - 1], *quad(k)[1],
        )

    def passing(p, k):
        came = misfit.at[p, core * QUADS + quad(k)[0]]
        return remote(came, came, s4, r4.at[p], *partner)

    def reduce_out(p):
        across(p).wait_recv()
        for k in (3, 1, 2):
            other = quad(k)[0]
            sums[p, k - 1] = (
                partial[p, core * QUADS + other].astype(f32) + first_in[p, other].astype(f32)
            ).astype(bf16)
            away(p, k).start()

    def compare(p):
        remote(sums.at[p], second_in.at[p], s2, r2.at[p], *partner).wait_recv()
        lanes = pl.ds(pl.multiple_of(p * strip, strip), strip)

        def whole(lo, hi):
            value = partial[p, mine, lo:hi].astype(f32) + first_in[p, q, lo:hi].astype(f32)
            for k in range(1, QUADS):
                value = value + second_in[p, k - 1, lo:hi].astype(f32)
            return value

        all_targets = targets[:, lanes].astype(f32)
        pool_row = lax.broadcasted_iota(jnp.int32, all_targets.shape, 0)
        tail_row = lax.broadcasted_iota(jnp.int32, (PAD, strip), 0)
        tail = jnp.zeros((PAD, strip), f32)
        outputs = whole(rows, rows + PAD)
        for i in range(spt):
            lo, hi = i * tangents, (i + 1) * tangents
            index = plan[0, sec * spt + i]
            misfit[p, mine, lo:hi] = (
                jacobian_weight * (whole(lo, hi) - jac[index, :, lanes].astype(f32))
            ).astype(bf16)
            target = jnp.sum(
                jnp.where(pool_row == index, all_targets, 0.0), axis=0, keepdims=True
            )
            tail = jnp.where(tail_row == mine * spt + i, outputs - target, tail)
        misfit[p, mine, rows:] = tail.astype(bf16)
        for k in (3, 1, 2, 0):
            gather(p, k).start()

    def pass_on(p):
        for k in (1, 2, 3):
            gather(p, k).wait_recv()
            passing(p, k).start()

    def others_in(p):
        theirs = misfit.at[p, pl.ds(pl.multiple_of((1 - core) * QUADS, QUADS), QUADS)]
        remote(theirs, theirs, s4, r4.at[p], *partner).wait_recv()

    def last_of(p):
        others_in(p)
        lhs = jnp.concatenate([misfit[p, b, 0:rows] for b in range(2 * QUADS)], axis=0)
        value = lax.dot_general(lhs, act[...], over_rows, preferred_element_type=f32)
        tail = misfit[p, 0, rows:].astype(f32)
        for b in range(1, 2 * QUADS):
            tail = tail + misfit[p, b, rows:].astype(f32)
        value = value + lax.dot_general(
            tail.astype(bf16), hidden[...], over_rows, preferred_element_type=f32
        )
        here = pl.ds(pl.multiple_of(p * strip, strip), strip)
        last_total[here, :] = value
        last_grads[here, :] = value.astype(bf16)

    def slab_of(o):
        return pl.ds(pl.multiple_of(o * slab, slab), slab)

    def last_link(j, kind, source=None, o=None):
        here = slice(j * lw, (j + 1) * lw)
        if source is None:
            o = others[kind] if not line else mate
            slab_at = o if not line else order[min(kind, 2)]
            source = last_grads.at[slab_of(slab_at), here]
        i = j * last_inbox.shape[0] + kind
        return remote(
            source, last_inbox.at[kind, :, here], s5, r5.at[i], o * GROUP + g, sec
        )

    def link(j, kind, source=None, o=None):
        if source is None:
            o = others[kind] if not line else mate
            slab_at = o if not line else order[min(kind, 2)]
            source = grads.at[j, slab_of(slab_at), :]
        i = j * inbox.shape[1] + kind
        return remote(source, inbox.at[j, kind], s6, r6.at[i], o * GROUP + g, sec)

    if line:
        turns = [(0, far_end, 3, across_z), (1, far_mid, 4, across_z), (3, mate, 2, mate)]

    def last_onward(j, r):
        return last_link(
            j, turns[r][2], last_halves.at[r, :, slice(j * lw, (j + 1) * lw)], turns[r][3]
        )

    def last_relay(j, r):
        @pl.when(middle)
        def _():
            kind, o, _, _ = turns[r]
            here = slice(j * lw, (j + 1) * lw)
            last_link(j, kind).wait_recv()
            last_halves[r, :, here] = (
                last_total[slab_of(o), here] + last_inbox[kind, :, here].astype(f32)
            ).astype(bf16)
            last_onward(j, r).start()

    def onward(j, r):
        return link(j, turns[r][2], halves.at[j, r], turns[r][3])

    def relay(j, r):
        @pl.when(middle)
        def _():
            kind, o, _, _ = turns[r]
            link(j, kind).wait_recv()
            halves[j, r] = (
                total[j, slab_of(o), :] + inbox[j, kind].astype(f32)
            ).astype(bf16)
            onward(j, r).start()

    def from_end(copies):
        @pl.when(jnp.logical_not(middle))
        def _():
            for copy in copies:
                copy.start()

    def columns(j):
        start = pl.multiple_of((sec * GROUP + g) * cols + j * zw, zw)
        return out.at[:, pl.ds(start, zw)]

    def keep(j):
        return pltpu.make_async_copy(finished.at[sec, j, g], columns(j), local.at[3])

    def hand(layer, j, k):
        h = lax.rem(g + k, GROUP)
        return remote(finished.at[layer, j, h], columns(j), s7, r7, base + h, layer)

    def add_up(layer, j, kinds):
        for h in range(GROUP):
            start = pl.multiple_of(s * slab + h * own_rows, own_rows)
            here = slice(h * own_rows, (h + 1) * own_rows)
            if layer:
                lo, hi = j * zw, (j + 1) * zw
                value = last_total[pl.ds(start, own_rows), lo:hi]
                for k in kinds:
                    value = value + last_inbox[k, here, lo:hi].astype(f32)
            else:
                value = total[j, pl.ds(start, own_rows), :]
                for k in kinds:
                    value = value + inbox[j, k, here, :].astype(f32)
            finished[layer, j, h] = value.astype(bf16)

    def finish(layer, j):
        if line:

            @pl.when(middle)
            def _():
                add_up(layer, j, (2, 4))

            @pl.when(jnp.logical_not(middle))
            def _():
                add_up(layer, j, (2,))
        else:
            add_up(layer, j, range(n_s - 1))
        for k in range(1, GROUP):
            hand(layer, j, k).start()

        @pl.when(sec != layer)
        def _():
            hand(layer, j, 0).start()

        @pl.when(sec == layer)
        def _():
            keep(j).start()

    def landed(j, one):
        if line:
            one(j, 2).wait_recv()

            @pl.when(middle)
            def _():
                one(j, 4).wait_recv()
        else:
            for k in range(n_s - 1):
                one(j, k).wait_recv()

    def arrived(j):
        landed(j, link)

    def backward(j):
        lo, hi = j * cw, (j + 1) * cw

        def pull(i, carry):
            lhs = jnp.concatenate(
                [
                    jnp.concatenate(
                        [misfit[p, i * QUADS + b, 0:rows] for p in range(STRIPS)], axis=1
                    )
                    for b in range(QUADS)
                ],
                axis=0,
            )
            cot = jnp.dot(lhs, both[1, :, lo:hi], preferred_element_type=f32)
            start = pl.multiple_of(i * loop_rows, loop_rows)
            for t in range(loop_samples):
                part = cot[t * tangents : (t + 1) * tangents]
                here = pl.ds(pl.multiple_of(start + t * tangents, tangents), tangents)
                slope = first[pl.ds(i * loop_samples + t, 1), lo:hi]
                proj[pl.ds(i * loop_samples + t, 1), :] = jnp.sum(
                    part * picked[here, lo:hi].astype(f32), axis=0, keepdims=True
                )
                pulled[here, :] = (part * slope).astype(bf16)
            return carry

        lax.fori_loop(0, n_loop, pull, 0)
        tail = jnp.zeros((PAD, reduced), f32)
        for b in range(2 * QUADS):
            tail = tail + jnp.concatenate(
                [misfit[p, b, rows:] for p in range(STRIPS)], axis=1
            ).astype(f32)
        cot = jnp.dot(tail.astype(bf16), both[1, :, lo:hi], preferred_element_type=f32)
        pre = (cot * first[:, lo:hi] + second[:, lo:hi] * proj[...]).astype(bf16)
        value = jnp.dot(onehot[...], pulled[...], preferred_element_type=f32)
        value = value + lax.dot_general(
            xs[...].astype(bf16), pre, over_rows, preferred_element_type=f32
        )
        for i in range(cw // zw):
            total[j * (cw // zw) + i] = value[:, i * zw : (i + 1) * zw]
            grads[j * (cw // zw) + i] = value[:, i * zw : (i + 1) * zw].astype(bf16)

    def own_strip():
        lhs = jnp.concatenate(
            [misfit[order[3], b, 0:rows] for b in range(2 * QUADS)], axis=0
        )
        value = lax.dot_general(lhs, act[...], over_rows, preferred_element_type=f32)
        tail = misfit[order[3], 0, rows:].astype(f32)
        for b in range(1, 2 * QUADS):
            tail = tail + misfit[order[3], b, rows:].astype(f32)
        last_total[slab_of(s), :] = value + lax.dot_general(
            tail.astype(bf16), hidden[...], over_rows, preferred_element_type=f32
        )

    def onehots():
        for t in range(n_all):
            deep = lax.broadcasted_iota(jnp.int32, (reduced, tangents), 0).astype(f32)
            onehot[:, t * tangents : (t + 1) * tangents] = (
                (deep == dirs[t : t + 1, :]).astype(f32).astype(bf16)
            )

    for i in range(2):
        partials(pairs[i], 1 - core)
        across(order[2 * i]).start()
        across(order[2 * i + 1]).start()
        partials(pairs[i], core)
        if i == 0:
            reduce_out(order[0])
            reduce_out(order[1])
    onehots()
    load_jac.wait()
    compare(order[0])
    compare(order[1])
    reduce_out(order[2])
    reduce_out(order[3])
    pass_on(order[0])
    last_of(order[0])
    if line:
        from_end([last_link(j, 0) for j in range(LASTS)])
    pass_on(order[1])
    last_of(order[1])
    if line:
        from_end([last_link(j, 1) for j in range(LASTS)])
    compare(order[2])
    if line:
        last_relay(0, 0)
    compare(order[3])
    if line:
        for j in range(1, LASTS):
            last_relay(j, 0)
    pass_on(order[2])
    last_of(order[2])
    if line:
        from_end([last_link(j, 2) for j in range(LASTS)])
    pass_on(order[3])
    per_chunk = LINKS // CHUNKS
    if line:
        last_relay(0, 1)
        others_in(order[3])
        last_relay(0, 2)
        for j in range(CHUNKS):
            backward(j)
            pieces = range(j * per_chunk, (j + 1) * per_chunk)
            from_end([link(i, k) for k in range(2) for i in pieces])
            if j == 0:
                for i in range(1, LASTS):
                    last_relay(i, 1)
                    last_relay(i, 2)
            if j == 2:
                for r in range(2):
                    for i in range(2):
                        relay(i, r)
        from_end([link(i, 2) for i in range(LINKS)])
        def pass_along(*pieces):
            for r in range(2):
                for i in pieces:
                    relay(i, r)

        def bring_back(*pieces):
            for i in pieces:
                relay(i, 2)

        pass_along(2, 3)
        bring_back(0, 1)
        own_strip()
        pass_along(4, 5)
        bring_back(2)
        for i in range(LASTS):
            landed(i, last_link)
        for j in range(LINKS):
            finish(1, j)
        relay(6, 0)
        relay(7, 0)
        bring_back(3)
        relay(6, 1)
        relay(7, 1)
        bring_back(4, 5, 6, 7)
        for j in range(LINKS):
            arrived(j)
            finish(0, j)
    else:
        last_of(order[3])
        for kind in range(n_s - 1):
            for j in range(LASTS):
                last_link(j, kind).start()
        for j in range(CHUNKS):
            backward(j)
            for kind in range(n_s - 1):
                for i in range(j * per_chunk, (j + 1) * per_chunk):
                    link(i, kind).start()
        for i in range(LASTS):
            landed(i, last_link)
        for j in range(LINKS):
            finish(1, j)
        for j in range(LINKS):
            arrived(j)
            finish(0, j)

    def all_sent(ref, send):
        remote(ref, ref, send, precv, *partner).wait_send()

    all_sent(packs.at[0 : GROUP - 1], psend)
    all_sent(mail.at[0 : (PIECES + 1) * side * pw // cols], wsend)
    all_sent(mail.at[0 : (PIECES - 1) * side * pw // cols], zsend)
    all_sent(first_in, s1)
    all_sent(second_in, s2)
    all_sent(second_in, s3)
    all_sent(first_in, s4)
    all_sent(last_halves if line else last_inbox, s5)
    all_sent(halves if line else inbox, s6)
    rest = out.at[:, 0 : (2 * GROUP - 1) * cols]
    all_sent(rest, s7)
    own_kept = finished.at[0, :, 0]
    pltpu.make_async_copy(own_kept, own_kept, local.at[3]).wait()
    remote(rest, rest, s7, r7, *partner).wait_recv()


def shards(n_dp, n_sec, samples, targets, jacobian_targets, directions, plan, weights):
    _, reduced, width = weights.shape
    pool, tangents = directions.shape
    team = n_sec * GROUP
    cols = width // team
    n_s = n_dp // GROUP
    spt = MICRO // n_sec
    rows = spt * tangents
    high = rows + PAD
    every = team * spt
    strip = reduced // STRIPS
    slab = reduced // n_s
    cw, zw = cols // CHUNKS, cols // LINKS
    kinds = 5 if n_s == 4 else n_s - 1
    f32, bf16 = jnp.float32, jnp.bfloat16
    vmem = pltpu.VMEM
    dma = lambda n: pltpu.SemaphoreType.DMA((n,))
    one = pltpu.SemaphoreType.DMA
    result = pl.pallas_call(
        functools.partial(fused_kernel, n_s),
        out_shape=jax.ShapeDtypeStruct((reduced // n_dp, width), bf16),
        in_specs=[pl.BlockSpec(memory_space=pltpu.SMEM)] + [ANY] * 5,
        out_specs=ANY,
        scratch_shapes=[
            vmem(samples.shape, bf16),
            vmem(directions.shape, jnp.int32),
            vmem(targets.shape, bf16),
            vmem((GROUP, pool, reduced + tangents), f32),
            vmem((n_sec, reduced, cols), bf16),
            vmem((reduced, cols), bf16),
            vmem(jacobian_targets.shape, bf16),
            vmem((every, reduced), f32),
            vmem((every, tangents), f32),
            vmem((every * tangents, reduced), bf16),
            vmem((reduced, every * tangents), bf16),
            vmem((every * tangents, cols), bf16),
            vmem((every, cols), bf16),
            vmem((every * tangents, cols), bf16),
            vmem((every, cols), f32),
            vmem((every, cols), f32),
            vmem((STRIPS, team, high, strip), bf16),
            vmem((STRIPS, QUADS, high, strip), bf16),
            vmem((STRIPS, QUADS - 1, high, strip), bf16),
            vmem((STRIPS, QUADS - 1, high, strip), bf16),
            vmem((STRIPS, team, high, strip), bf16),
            vmem((LINKS, reduced, zw), f32),
            vmem((LINKS, reduced, zw), bf16),
            vmem((LINKS, kinds, slab, zw), bf16),
            vmem((LINKS, 3, slab, zw), bf16),
            vmem((reduced, cols), f32),
            vmem((reduced, cols), bf16),
            vmem((kinds, slab, cols), bf16),
            vmem((3, slab, cols), bf16),
            vmem((every * tangents, cw), bf16),
            vmem((every, cw), f32),
            vmem((n_sec, LINKS, GROUP, reduced // n_dp, zw), bf16),
            one, one, one, dma(PIECES + 1), one, dma(PIECES - 1),
            one, dma(STRIPS), one, dma(STRIPS), one, dma(STRIPS * 3), one, dma(STRIPS),
            one, dma(LASTS * kinds), one, dma(LINKS * kinds), one, one, dma(7),
        ],
        compiler_params=pltpu.CompilerParams(
            collective_id=0, has_side_effects=True, vmem_limit_bytes=60 * 1024 * 1024
        ),
        name="fused",
    )(plan, samples, directions, targets, jacobian_targets, weights)
    return result.astype(f32)[None]


def solution(mesh):
    placed = (
        P("dp", None),
        P("dp", None),
        P("dp", None, None),
        P("dp", None),
        P("dp", None),
        P("section", None, None),
    )
    body = functools.partial(shards, mesh.shape["dp"], mesh.shape["section"])
    return jax.shard_map(
        body, mesh=mesh, in_specs=placed, out_specs=P("section", "dp", None), check_vma=False
    )
```

```python
import functools

import jax
import jax.numpy as jnp
from jax import lax
from jax.experimental import pallas as pl
from jax.experimental.pallas import tpu as pltpu
from jax.sharding import PartitionSpec as P

MICRO = 4
GROUP = 4
PAD = 16
PIECES = 8
CHUNKS = 4
STRIPS = 4
LINKS = 8
LASTS = 2
QUADS = 4

jacobian_weight = 32.0

ANY = pl.BlockSpec(memory_space=pl.ANY)


def remote(src, dst, send, recv, dp, sec):
    return pltpu.make_async_remote_copy(
        src_ref=src, dst_ref=dst, send_sem=send, recv_sem=recv,
        device_id={"dp": dp, "section": sec},
    )


def fused_kernel(
    n_s, plan, samples_hbm, directions_hbm, targets_hbm, jac_hbm, weight, out,
    samples, directions, targets, packs, both, mail, jac, xs, dirs, onehot_t, onehot, act, hidden, picked, first, second,
    partial, first_in, sums, second_in, misfit, total, grads, inbox, halves,
    last_total, last_grads, last_inbox, last_halves, pulled, proj, finished,
    psend, precv, wsend, wrecv, zsend, zrecv, s1, r1, s2, r2, s3, r3, s4, r4,
    s5, r5, s6, r6, s7, r7, local,
):
    f32, bf16 = jnp.float32, jnp.bfloat16
    dp, sec = lax.axis_index("dp"), lax.axis_index("section")
    g = lax.rem(dp, GROUP)
    base = dp - g
    s = dp // GROUP
    core, half = lax.rem(g, 2), g // 2
    q = sec * 2 + half
    mine = core * QUADS + q
    partner = (base + half * 2 + (1 - core), sec)
    parity = lax.rem(s, 2)
    mate = s + 1 - 2 * parity
    twin = (mate * GROUP + g, sec)
    line = n_s == 4
    reduced, cols = both.shape[1:]
    tangents = directions.shape[1]
    spt = MICRO // 2
    rows = spt * tangents
    strip = reduced // STRIPS
    slab = reduced // n_s
    own_rows = slab // GROUP
    cw = cols // CHUNKS
    pw = cols // PIECES
    zw = cols // LINKS
    lw = cols // LASTS
    over_rows = (((0,), (0,)), ((), ()))
    over_cols = (((1,), (1,)), ((), ()))

    def quad(k):
        l = 1 - sec if k & 2 else sec
        h = 1 - half if k & 1 else half
        return l * 2 + h, (base + h * 2 + core, l)

    if line:
        far_end, far_mid, across_z = 3 - 3 * (s // 2), 2 - s // 2, 3 - s
        middle = lax.rem(s + 1, 4) >= 2
        others = [mate]
        order = [far_end, far_mid, mate, s]
        pairs = [1 - s // 2, s // 2]
    else:
        others = [lax.rem(s + k, n_s) for k in range(1, n_s)]
        order = list(range(STRIPS))
        pairs = [0, 1]

    far_start = pl.multiple_of(((1 - sec) * GROUP + g) * cols, cols)
    load_mail = pltpu.make_async_copy(
        weight.at[0, :, pl.ds(far_start, cols)], mail, local.at[2]
    )
    load_mail.start()
    own = pltpu.make_async_copy(
        weight.at[0, :, pl.ds(pl.multiple_of((sec * GROUP + g) * cols, cols), cols)],
        both.at[sec], local.at[0],
    )
    own.start()
    load_jac = pltpu.make_async_copy(jac_hbm, jac, local.at[1])
    load_jac.start()
    loads = [
        pltpu.make_async_copy(a, b, local.at[4 + i])
        for i, (a, b) in enumerate(
            ((samples_hbm, samples), (directions_hbm, directions), (targets_hbm, targets))
        )
    ]
    for copy in loads:
        copy.start()

    barrier = pltpu.get_barrier_semaphore()
    peers = [
        (base + lax.rem(g + k, GROUP), 1 - sec if j else sec)
        for j in range(2) for k in range(GROUP) if j or k
    ] + [(o * GROUP + g, sec) for o in others]
    for d, l in peers:
        pl.semaphore_signal(barrier, inc=1, device_id={"dp": d, "section": l})
    if line:

        @pl.when(middle)
        def _():
            pl.semaphore_signal(
                barrier, inc=1, device_id={"dp": across_z * GROUP + g, "section": sec}
            )

    pl.semaphore_wait(barrier, len(peers) + (jnp.where(middle, 1, 0) if line else 0))


    side = reduced // 2
    half_rows = pl.ds(pl.multiple_of(parity * side, side), side)
    other_rows = pl.ds(pl.multiple_of((1 - parity) * side, side), side)
    load_mail.wait()
    sent, relayed = [], []
    for c in range(PIECES + 1):
        here = (half_rows if c < PIECES else other_rows, pl.ds(min(c, PIECES - 1) * pw, pw))
        sent.append(remote(
            mail.at[here], both.at[(sec,) + here], wsend, wrecv.at[c], dp, 1 - sec,
        ))
        sent[-1].start()

    for copy in loads:
        copy.wait()
    every = jnp.concatenate(
        [samples[...].astype(f32), directions[...].astype(f32)], axis=1
    )
    row = lax.broadcasted_iota(jnp.int32, every.shape, 0)
    packed = jnp.zeros_like(every)
    for k in range(MICRO):
        chosen = jnp.sum(jnp.where(row == plan[0, k], every, 0.0), axis=0, keepdims=True)
        packed = jnp.where(row == k, chosen, packed)
    packs[g] = packed
    shared = []
    for k in range(1, GROUP):
        shared.append(remote(
            packs.at[g], packs.at[g], psend, precv,
            base + lax.rem(g + k, GROUP), sec,
        ))
        shared[-1].start()

    def arrive(c):
        sent[c].wait_recv()
        if c < PIECES - 1:
            came = both.at[1 - sec, half_rows, pl.ds(c * pw, pw)]
            relayed.append(remote(came, came, zsend, zrecv.at[c], *twin))
            relayed[-1].start()

    arrive(0)
    several = packs.at[0 : GROUP - 1]
    remote(several, several, psend, precv, *partner).wait_recv()
    for b in range(2 * QUADS):
        c, l, h = b // QUADS, (b % QUADS) // 2, b % 2
        xs[b * spt : (b + 1) * spt] = packs[h * 2 + c, l * spt : (l + 1) * spt, :reduced]
        dirs[b * spt : (b + 1) * spt] = packs[h * 2 + c, l * spt : (l + 1) * spt, reduced:]
    n_all = 2 * QUADS * spt
    turned = dirs[...].T

    def spread_directions(ts):
        for t in ts:
            lane = lax.broadcasted_iota(jnp.int32, (tangents, reduced), 1).astype(f32)
            onehot_t[t * tangents : (t + 1) * tangents] = (
                (lane == turned[:, t : t + 1]).astype(f32).astype(bf16)
            )

    arrive(1)
    spread_directions(range(n_all // 2))
    arrive(2)
    spread_directions(range(n_all // 2, n_all))
    arrive(3)

    n_loop = 2
    loop_rows = n_all * tangents // n_loop
    loop_samples = n_all // n_loop

    def forward(c):
        lo, hi = c * cw, (c + 1) * cw
        linear = jnp.dot(xs[...].astype(bf16), both[0, :, lo:hi], preferred_element_type=f32)
        squash = jax.nn.sigmoid(linear)
        first[:, lo:hi] = squash * (1.0 + linear * (1.0 - squash))
        second[:, lo:hi] = squash * (1.0 - squash) * (2.0 + linear * (1.0 - 2.0 * squash))
        hidden[:, lo:hi] = (linear * squash).astype(bf16)

        def pick(i, carry):
            start = pl.multiple_of(i * loop_rows, loop_rows)
            value = jnp.dot(
                onehot_t[pl.ds(start, loop_rows), :], both[0, :, lo:hi],
                preferred_element_type=f32,
            )
            picked[pl.ds(start, loop_rows), lo:hi] = value.astype(bf16)
            for t in range(loop_samples):
                slope = first[pl.ds(i * loop_samples + t, 1), lo:hi]
                here = pl.ds(pl.multiple_of(start + t * tangents, tangents), tangents)
                act[here, lo:hi] = (
                    slope * value[t * tangents : (t + 1) * tangents]
                ).astype(bf16)
            return carry

        lax.fori_loop(0, n_loop, pick, 0)

    own.wait()
    per_chunk = PIECES // CHUNKS
    for c in range(CHUNKS):
        for i in ([], [4, 5], [6], [7, 8])[c]:
            arrive(i)
        for i in range(c * per_chunk, min((c + 1) * per_chunk, PIECES - 1)):
            relayed[i].wait_recv()
        forward(c)

    def partials(pair, side):
        start = pl.multiple_of(pair * 2 * strip, 2 * strip)
        decoder = both[1, pl.ds(start, 2 * strip), :]
        lo = pl.multiple_of(side * (QUADS * rows), QUADS * rows)
        value = lax.dot_general(
            act[pl.ds(lo, QUADS * rows), :], decoder, over_cols, preferred_element_type=f32
        ).astype(bf16)
        tail = lax.dot_general(
            hidden[...], decoder, over_cols, preferred_element_type=f32
        ).astype(bf16)
        for i in range(2):
            a, b = i * strip, (i + 1) * strip
            for j in range(QUADS):
                partial[pair * 2 + i, side * QUADS + j, 0:rows] = (
                    value[j * rows : (j + 1) * rows, a:b]
                )
                partial[pair * 2 + i, side * QUADS + j, rows:] = tail[:, a:b]

    def across(p):
        theirs = pl.ds(pl.multiple_of((1 - core) * QUADS, QUADS), QUADS)
        return remote(
            partial.at[p, theirs], first_in.at[p], s1, r1.at[p], *partner
        )

    def away(p, k):
        return remote(
            sums.at[p, k - 1], second_in.at[p, k - 1],
            s2, r2.at[p], *quad(k)[1],
        )

    def gather(p, k):
        if k == 0:
            return remote(
                misfit.at[p, mine], misfit.at[p, mine], s4, r4.at[p], *partner
            )
        return remote(
            misfit.at[p, mine], misfit.at[p, mine],
            s3, r3.at[p * 3 + k - 1], *quad(k)[1],
        )

    def passing(p, k):
        came = misfit.at[p, core * QUADS + quad(k)[0]]
        return remote(came, came, s4, r4.at[p], *partner)

    def reduce_out(p):
        across(p).wait_recv()
        for k in (3, 1, 2):
            other = quad(k)[0]
            sums[p, k - 1] = (
                partial[p, core * QUADS + other].astype(f32) + first_in[p, other].astype(f32)
            ).astype(bf16)
            away(p, k).start()

    def compare(p):
        remote(sums.at[p], second_in.at[p], s2, r2.at[p], *partner).wait_recv()
        lanes = pl.ds(pl.multiple_of(p * strip, strip), strip)

        def whole(lo, hi):
            value = partial[p, mine, lo:hi].astype(f32) + first_in[p, q, lo:hi].astype(f32)
            for k in range(1, QUADS):
                value = value + second_in[p, k - 1, lo:hi].astype(f32)
            return value

        all_targets = targets[:, lanes].astype(f32)
        pool_row = lax.broadcasted_iota(jnp.int32, all_targets.shape, 0)
        tail_row = lax.broadcasted_iota(jnp.int32, (PAD, strip), 0)
        tail = jnp.zeros((PAD, strip), f32)
        outputs = whole(rows, rows + PAD)
        for i in range(spt):
            lo, hi = i * tangents, (i + 1) * tangents
            index = plan[0, sec * spt + i]
            misfit[p, mine, lo:hi] = (
                jacobian_weight * (whole(lo, hi) - jac[index, :, lanes].astype(f32))
            ).astype(bf16)
            target = jnp.sum(
                jnp.where(pool_row == index, all_targets, 0.0), axis=0, keepdims=True
            )
            tail = jnp.where(tail_row == mine * spt + i, outputs - target, tail)
        misfit[p, mine, rows:] = tail.astype(bf16)
        for k in (3, 1, 2, 0):
            gather(p, k).start()

    def pass_on(p):
        for k in (1, 2, 3):
            gather(p, k).wait_recv()
            passing(p, k).start()

    def others_in(p):
        theirs = misfit.at[p, pl.ds(pl.multiple_of((1 - core) * QUADS, QUADS), QUADS)]
        remote(theirs, theirs, s4, r4.at[p], *partner).wait_recv()

    def last_of(p):
        others_in(p)
        lhs = jnp.concatenate([misfit[p, b, 0:rows] for b in range(2 * QUADS)], axis=0)
        value = lax.dot_general(lhs, act[...], over_rows, preferred_element_type=f32)
        tail = misfit[p, 0, rows:].astype(f32)
        for b in range(1, 2 * QUADS):
            tail = tail + misfit[p, b, rows:].astype(f32)
        value = value + lax.dot_general(
            tail.astype(bf16), hidden[...], over_rows, preferred_element_type=f32
        )
        here = pl.ds(pl.multiple_of(p * strip, strip), strip)
        last_total[here, :] = value
        last_grads[here, :] = value.astype(bf16)

    def slab_of(o):
        return pl.ds(pl.multiple_of(o * slab, slab), slab)

    def last_link(j, kind, source=None, o=None):
        here = slice(j * lw, (j + 1) * lw)
        if source is None:
            o = others[kind] if not line else mate
            slab_at = o if not line else order[min(kind, 2)]
            source = last_grads.at[slab_of(slab_at), here]
        i = j * last_inbox.shape[0] + kind
        return remote(
            source, last_inbox.at[kind, :, here], s5, r5.at[i], o * GROUP + g, sec
        )

    def link(j, kind, source=None, o=None):
        if source is None:
            o = others[kind] if not line else mate
            slab_at = o if not line else order[min(kind, 2)]
            source = grads.at[j, slab_of(slab_at), :]
        i = j * inbox.shape[1] + kind
        return remote(source, inbox.at[j, kind], s6, r6.at[i], o * GROUP + g, sec)

    if line:
        turns = [(0, far_end, 3, across_z), (1, far_mid, 4, across_z), (3, mate, 2, mate)]

    def last_onward(j, r):
        return last_link(
            j, turns[r][2], last_halves.at[r, :, slice(j * lw, (j + 1) * lw)], turns[r][3]
        )

    def last_relay(j, r):
        @pl.when(middle)
        def _():
            kind, o, _, _ = turns[r]
            here = slice(j * lw, (j + 1) * lw)
            last_link(j, kind).wait_recv()
            last_halves[r, :, here] = (
                last_total[slab_of(o), here] + last_inbox[kind, :, here].astype(f32)
            ).astype(bf16)
            last_onward(j, r).start()

    def onward(j, r):
        return link(j, turns[r][2], halves.at[j, r], turns[r][3])

    def relay(j, r):
        @pl.when(middle)
        def _():
            kind, o, _, _ = turns[r]
            link(j, kind).wait_recv()
            halves[j, r] = (
                total[j, slab_of(o), :] + inbox[j, kind].astype(f32)
            ).astype(bf16)
            onward(j, r).start()

    def from_end(copies):
        @pl.when(jnp.logical_not(middle))
        def _():
            for copy in copies:
                copy.start()

    def columns(j):
        start = pl.multiple_of((sec * GROUP + g) * cols + j * zw, zw)
        return out.at[:, pl.ds(start, zw)]

    def keep(j):
        return pltpu.make_async_copy(finished.at[sec, j, g], columns(j), local.at[3])

    def hand(layer, j, k):
        h = lax.rem(g + k, GROUP)
        return remote(finished.at[layer, j, h], columns(j), s7, r7, base + h, layer)

    def add_up(layer, j, kinds):
        for h in range(GROUP):
            start = pl.multiple_of(s * slab + h * own_rows, own_rows)
            here = slice(h * own_rows, (h + 1) * own_rows)
            if layer:
                lo, hi = j * zw, (j + 1) * zw
                value = last_total[pl.ds(start, own_rows), lo:hi]
                for k in kinds:
                    value = value + last_inbox[k, here, lo:hi].astype(f32)
            else:
                value = total[j, pl.ds(start, own_rows), :]
                for k in kinds:
                    value = value + inbox[j, k, here, :].astype(f32)
            finished[layer, j, h] = value.astype(bf16)

    def finish(layer, j):
        if line:

            @pl.when(middle)
            def _():
                add_up(layer, j, (2, 4))

            @pl.when(jnp.logical_not(middle))
            def _():
                add_up(layer, j, (2,))
        else:
            add_up(layer, j, range(n_s - 1))
        for k in range(1, GROUP):
            hand(layer, j, k).start()

        @pl.when(sec != layer)
        def _():
            hand(layer, j, 0).start()

        @pl.when(sec == layer)
        def _():
            keep(j).start()

    def landed(j, one):
        if line:
            one(j, 2).wait_recv()

            @pl.when(middle)
            def _():
                one(j, 4).wait_recv()
        else:
            for k in range(n_s - 1):
                one(j, k).wait_recv()

    def arrived(j):
        landed(j, link)

    def backward(j):
        lo, hi = j * cw, (j + 1) * cw

        def pull(i, carry):
            lhs = jnp.concatenate(
                [
                    jnp.concatenate(
                        [misfit[p, i * QUADS + b, 0:rows] for p in range(STRIPS)], axis=1
                    )
                    for b in range(QUADS)
                ],
                axis=0,
            )
            cot = jnp.dot(lhs, both[1, :, lo:hi], preferred_element_type=f32)
            start = pl.multiple_of(i * loop_rows, loop_rows)
            for t in range(loop_samples):
                part = cot[t * tangents : (t + 1) * tangents]
                here = pl.ds(pl.multiple_of(start + t * tangents, tangents), tangents)
                slope = first[pl.ds(i * loop_samples + t, 1), lo:hi]
                proj[pl.ds(i * loop_samples + t, 1), :] = jnp.sum(
                    part * picked[here, lo:hi].astype(f32), axis=0, keepdims=True
                )
                pulled[here, :] = (part * slope).astype(bf16)
            return carry

        lax.fori_loop(0, n_loop, pull, 0)
        tail = jnp.zeros((PAD, reduced), f32)
        for b in range(2 * QUADS):
            tail = tail + jnp.concatenate(
                [misfit[p, b, rows:] for p in range(STRIPS)], axis=1
            ).astype(f32)
        cot = jnp.dot(tail.astype(bf16), both[1, :, lo:hi], preferred_element_type=f32)
        pre = (cot * first[:, lo:hi] + second[:, lo:hi] * proj[...]).astype(bf16)
        value = jnp.dot(onehot[...], pulled[...], preferred_element_type=f32)
        value = value + lax.dot_general(
            xs[...].astype(bf16), pre, over_rows, preferred_element_type=f32
        )
        for i in range(cw // zw):
            total[j * (cw // zw) + i] = value[:, i * zw : (i + 1) * zw]
            grads[j * (cw // zw) + i] = value[:, i * zw : (i + 1) * zw].astype(bf16)

    def own_strip():
        lhs = jnp.concatenate(
            [misfit[order[3], b, 0:rows] for b in range(2 * QUADS)], axis=0
        )
        value = lax.dot_general(lhs, act[...], over_rows, preferred_element_type=f32)
        tail = misfit[order[3], 0, rows:].astype(f32)
        for b in range(1, 2 * QUADS):
            tail = tail + misfit[order[3], b, rows:].astype(f32)
        last_total[slab_of(s), :] = value + lax.dot_general(
            tail.astype(bf16), hidden[...], over_rows, preferred_element_type=f32
        )

    def onehots():
        for t in range(n_all):
            deep = lax.broadcasted_iota(jnp.int32, (reduced, tangents), 0).astype(f32)
            onehot[:, t * tangents : (t + 1) * tangents] = (
                (deep == dirs[t : t + 1, :]).astype(f32).astype(bf16)
            )

    for i in range(2):
        partials(pairs[i], 1 - core)
        across(order[2 * i]).start()
        across(order[2 * i + 1]).start()
        partials(pairs[i], core)
        if i == 0:
            reduce_out(order[0])
            reduce_out(order[1])
    onehots()
    load_jac.wait()
    compare(order[0])
    compare(order[1])
    reduce_out(order[2])
    reduce_out(order[3])
    pass_on(order[0])
    last_of(order[0])
    if line:
        from_end([last_link(j, 0) for j in range(LASTS)])
    pass_on(order[1])
    last_of(order[1])
    if line:
        from_end([last_link(j, 1) for j in range(LASTS)])
    compare(order[2])
    if line:
        last_relay(0, 0)
    compare(order[3])
    if line:
        for j in range(1, LASTS):
            last_relay(j, 0)
    pass_on(order[2])
    last_of(order[2])
    if line:
        from_end([last_link(j, 2) for j in range(LASTS)])
    pass_on(order[3])
    per_chunk = LINKS // CHUNKS
    if line:
        last_relay(0, 1)
        others_in(order[3])
        last_relay(0, 2)
        def pass_along(r, *pieces):
            for i in pieces:
                relay(i, r)

        for j in range(CHUNKS):
            backward(j)
            pieces = list(range(j * per_chunk, (j + 1) * per_chunk))
            before = [i - per_chunk for i in pieces if j]
            rest_too = j == CHUNKS - 1
            from_end(
                [link(i, 0) for i in pieces]
                + [link(i, 1) for i in before + (pieces if rest_too else [])]
                + [link(i, 2) for i in range(LINKS if rest_too else 0)]
            )
            if j == 0:
                for i in range(1, LASTS):
                    last_relay(i, 1)
                    last_relay(i, 2)
            if j == 2:
                pass_along(0, 0, 1)
        pass_along(0, 2, 3)
        pass_along(1, 0, 1)
        pass_along(0, 4, 5)
        pass_along(2, 0, 1)
        own_strip()
        pass_along(1, 2, 3)
        pass_along(0, 6, 7)
        pass_along(2, 2, 3)
        for i in range(LASTS):
            landed(i, last_link)
        for j in range(LINKS):
            finish(1, j)
        pass_along(1, 4, 5)
        pass_along(2, 4, 5)
        pass_along(1, 6, 7)
        pass_along(2, 6, 7)
        for j in range(LINKS):
            arrived(j)
            finish(0, j)
    else:
        last_of(order[3])
        for kind in range(n_s - 1):
            for j in range(LASTS):
                last_link(j, kind).start()
        for j in range(CHUNKS):
            backward(j)
            for kind in range(n_s - 1):
                for i in range(j * per_chunk, (j + 1) * per_chunk):
                    link(i, kind).start()
        for i in range(LASTS):
            landed(i, last_link)
        for j in range(LINKS):
            finish(1, j)
        for j in range(LINKS):
            arrived(j)
            finish(0, j)

    def all_sent(ref, send):
        remote(ref, ref, send, precv, *partner).wait_send()

    all_sent(packs.at[0 : GROUP - 1], psend)
    all_sent(mail.at[0 : (PIECES + 1) * side * pw // cols], wsend)
    all_sent(mail.at[0 : (PIECES - 1) * side * pw // cols], zsend)
    all_sent(first_in, s1)
    all_sent(second_in, s2)
    all_sent(second_in, s3)
    all_sent(first_in, s4)
    all_sent(last_halves if line else last_inbox, s5)
    all_sent(halves if line else inbox, s6)
    rest = out.at[:, 0 : (2 * GROUP - 1) * cols]
    all_sent(rest, s7)
    own_kept = finished.at[0, :, 0]
    pltpu.make_async_copy(own_kept, own_kept, local.at[3]).wait()
    remote(rest, rest, s7, r7, *partner).wait_recv()


def shards(n_dp, n_sec, samples, targets, jacobian_targets, directions, plan, weights):
    _, reduced, width = weights.shape
    pool, tangents = directions.shape
    team = n_sec * GROUP
    cols = width // team
    n_s = n_dp // GROUP
    spt = MICRO // n_sec
    rows = spt * tangents
    high = rows + PAD
    every = team * spt
    strip = reduced // STRIPS
    slab = reduced // n_s
    cw, zw = cols // CHUNKS, cols // LINKS
    kinds = 5 if n_s == 4 else n_s - 1
    f32, bf16 = jnp.float32, jnp.bfloat16
    vmem = pltpu.VMEM
    dma = lambda n: pltpu.SemaphoreType.DMA((n,))
    one = pltpu.SemaphoreType.DMA
    result = pl.pallas_call(
        functools.partial(fused_kernel, n_s),
        out_shape=jax.ShapeDtypeStruct((reduced // n_dp, width), bf16),
        in_specs=[pl.BlockSpec(memory_space=pltpu.SMEM)] + [ANY] * 5,
        out_specs=ANY,
        scratch_shapes=[
            vmem(samples.shape, bf16),
            vmem(directions.shape, jnp.int32),
            vmem(targets.shape, bf16),
            vmem((GROUP, pool, reduced + tangents), f32),
            vmem((n_sec, reduced, cols), bf16),
            vmem((reduced, cols), bf16),
            vmem(jacobian_targets.shape, bf16),
            vmem((every, reduced), f32),
            vmem((every, tangents), f32),
            vmem((every * tangents, reduced), bf16),
            vmem((reduced, every * tangents), bf16),
            vmem((every * tangents, cols), bf16),
            vmem((every, cols), bf16),
            vmem((every * tangents, cols), bf16),
            vmem((every, cols), f32),
            vmem((every, cols), f32),
            vmem((STRIPS, team, high, strip), bf16),
            vmem((STRIPS, QUADS, high, strip), bf16),
            vmem((STRIPS, QUADS - 1, high, strip), bf16),
            vmem((STRIPS, QUADS - 1, high, strip), bf16),
            vmem((STRIPS, team, high, strip), bf16),
            vmem((LINKS, reduced, zw), f32),
            vmem((LINKS, reduced, zw), bf16),
            vmem((LINKS, kinds, slab, zw), bf16),
            vmem((LINKS, 3, slab, zw), bf16),
            vmem((reduced, cols), f32),
            vmem((reduced, cols), bf16),
            vmem((kinds, slab, cols), bf16),
            vmem((3, slab, cols), bf16),
            vmem((every * tangents, cw), bf16),
            vmem((every, cw), f32),
            vmem((n_sec, LINKS, GROUP, reduced // n_dp, zw), bf16),
            one, one, one, dma(PIECES + 1), one, dma(PIECES - 1),
            one, dma(STRIPS), one, dma(STRIPS), one, dma(STRIPS * 3), one, dma(STRIPS),
            one, dma(LASTS * kinds), one, dma(LINKS * kinds), one, one, dma(7),
        ],
        compiler_params=pltpu.CompilerParams(
            collective_id=0, has_side_effects=True, vmem_limit_bytes=60 * 1024 * 1024
        ),
        name="fused",
    )(plan, samples, directions, targets, jacobian_targets, weights)
    return result.astype(f32)[None]


def solution(mesh):
    placed = (
        P("dp", None),
        P("dp", None),
        P("dp", None, None),
        P("dp", None),
        P("dp", None),
        P("section", None, None),
    )
    body = functools.partial(shards, mesh.shape["dp"], mesh.shape["section"])
    return jax.shard_map(
        body, mesh=mesh, in_specs=placed, out_specs=P("section", "dp", None), check_vma=False
    )
```
